32 devices in a mesh: slab: 16 (over z, y, x), cell: 2 (over core).
Axes of the slice: x: 2, y: 2, z: 4, core: 2. Of those that a mesh axis runs over, the one named last changes fastest.
Arguments:
- cell_row: int32 [16384], P(('slab', 'cell')), may hold values from 0 to 2043, as said below
- cell_col: int32 [16384], P(('slab', 'cell')), may hold values from 0 to 2039
- cell_width: int32 [16384], P(('slab', 'cell')), may hold values from 1 to 8
- cell_height: int32 [16384], P(('slab', 'cell')), may hold values from 1 to 4
- cell_region: int32 [16384], P(('slab', 'cell')), may hold values from 0 to 3
- cell_offset: float32 [2, 16384], P(None, ('slab', 'cell')), may hold values from 0 to 1
Outputs:
- field_x: float32 [4, 2048, 2048], P(None, ('slab', 'cell'))
- field_y: float32 [4, 2048, 2048], P(None, ('slab', 'cell'))
- cell_force: float32 [2, 16384], P(None, ('slab', 'cell'))
- energy: float32 [], replicated
- overflow: float32 [], replicated
The draws below stay inside these ranges and needn't reach their ends.
Inputs may be any that keep to these rules, and one draw needn't show every extreme that they name: `cell_row`: cell i belongs to row slab s = i // 1024: its row lies in [s * 128, (s + 1) * 128); cells of the last slab lie at least 4 rows below the top of the grid.
All inputs are finite; a program needn't handle non-finite values.
Results may differ from the reference program's by a relative error of at most 0.0015.
Values may be sent and summed in bfloat16 or wider, within the bound.
A program may use at most 128 MiB of HBM per device.

```python
import jax
import jax.numpy as jnp
from jax import lax

M = 2048
REGIONS = 4
HMAX = 4
WMAX = 8
ROWS = 128
CELLS_SLAB = 1024
CELLS = 16384


def draw_cell_row(key, part):
    positions = jnp.arange(CELLS, dtype=jnp.int32)
    slab_index = positions // CELLS_SLAB
    top_slab = M // ROWS - 1
    row_room = jnp.where(slab_index == top_slab, ROWS - HMAX, ROWS)
    random_bits = jax.random.randint(key, (CELLS,), 0, 1 << 20, dtype=jnp.int32)
    offset_rows = jnp.where(positions == top_slab * CELLS_SLAB, row_room - 1, random_bits % row_room)
    return (slab_index * ROWS + offset_rows).astype(jnp.int32)


def draw_cell_width(key, part):
    slab_count = M // ROWS
    key_cap, key_pick, key_width = jax.random.split(jax.random.fold_in(key, 7), 3)
    slab_caps = 1 + jax.random.randint(key_cap, (slab_count,), 0, WMAX, dtype=jnp.int32)
    widest = jax.random.randint(key_pick, (), 0, slab_count, dtype=jnp.int32)
    slab_caps = jnp.where(jnp.arange(slab_count, dtype=jnp.int32) == widest, WMAX, slab_caps)
    positions = jnp.arange(CELLS, dtype=jnp.int32)
    owner_slab = positions // CELLS_SLAB
    random_bits = jax.random.randint(key_width, (CELLS,), 0, 1 << 20, dtype=jnp.int32)
    widths = 1 + random_bits % slab_caps[owner_slab]
    return jnp.where(positions == widest * CELLS_SLAB, WMAX, widths).astype(jnp.int32)


def set_ends(values, key, least, top_value):
    spot = [jax.random.randint(jax.random.fold_in(key, axis), (), 0, length) for axis, length in enumerate(values.shape)]
    widest = values.shape.index(max(values.shape))
    neighbour = spot[:widest] + [(spot[widest] + 1) % values.shape[widest]] + spot[widest + 1:]
    return values.at[tuple(spot)].set(least).at[tuple(neighbour)].set(top_value)


def block_scale(key, shape, cuts, low, largest):
    def one(axis_at, blocks):
        draws = jax.random.uniform(jax.random.fold_in(jax.random.fold_in(key, 6), axis_at), (blocks,), jnp.float32, low / len(cuts), largest / len(cuts))
        return jnp.repeat(jnp.exp(draws), shape[axis_at] // blocks).reshape((-1,) + (1,) * (len(shape) - axis_at - 1))

    gain = one(*cuts[0])
    for cut in cuts[1:]:
        gain = gain * one(*cut)
    return gain


def setup_inputs(seed: int = 0) -> dict:
    key_list = jax.random.split(jax.random.key(seed), 7)
    cell_row = draw_cell_row(jax.random.fold_in(key_list[6], 71), 0)
    cell_col = set_ends(jax.random.randint(key_list[1], (CELLS,), 0, M - WMAX), jax.random.fold_in(key_list[1], 1), 0, (M - WMAX) - 1).astype(jnp.int32)
    cell_width = draw_cell_width(jax.random.fold_in(key_list[6], 71), 0)
    cell_height = set_ends(jax.random.randint(key_list[3], (CELLS,), 1, HMAX + 1), jax.random.fold_in(key_list[3], 1), 1, HMAX).astype(jnp.int32)
    cell_region = set_ends(jax.random.randint(key_list[4], (CELLS,), 0, REGIONS), jax.random.fold_in(key_list[4], 1), 0, REGIONS - 1).astype(jnp.int32)
    cell_offset = jnp.clip(1.0 * jax.random.uniform(key_list[5], (2, CELLS), jnp.float32) ** block_scale(key_list[5], (2, CELLS), ((1, 32),), -0.2, 0.2), 0.0, 1.0)
    return dict(cell_row=cell_row, cell_col=cell_col, cell_width=cell_width, cell_height=cell_height, cell_region=cell_region, cell_offset=cell_offset)


def intersect(offset_bins, fraction, extent):
    high_edge = jnp.minimum(offset_bins + 1.0, fraction + extent)
    low_edge = jnp.maximum(offset_bins, fraction)
    return jnp.maximum(high_edge - low_edge, 0.0).astype(jnp.bfloat16)

def basis_weight(length):
    freq_index = jnp.arange(length)
    return jnp.where(freq_index == 0, jnp.sqrt(1.0 / length), jnp.sqrt(2.0 / length)).astype(jnp.float32)

def dct_forward(values, axis):
    length = values.shape[axis]
    moved = jnp.moveaxis(values, axis, -1)
    doubled = jnp.concatenate([moved, jnp.flip(moved, -1)], axis=-1)
    spectral = jnp.fft.fft(doubled, axis=-1)[..., :length]
    freq_axis = jnp.arange(length).astype(jnp.float32)
    twist = jnp.exp(-1j * (jnp.pi / (2 * length)) * freq_axis)
    result = jnp.real(spectral * twist) * (0.5 * basis_weight(length))
    return jnp.moveaxis(result, -1, axis)

def dct_inverse(values, axis, sine):
    length = values.shape[axis]
    moved = jnp.moveaxis(values, axis, -1)
    freq_axis = jnp.arange(length).astype(jnp.float32)
    twisted = moved * basis_weight(length) * jnp.exp(1j * (jnp.pi / (2 * length)) * freq_axis)
    padded = jnp.concatenate([twisted, jnp.zeros_like(twisted)], axis=-1)
    summed = jnp.fft.ifft(padded, axis=-1)[..., :length] * (2 * length)
    picked = jnp.imag(summed) if sine else jnp.real(summed)
    return jnp.moveaxis(picked, -1, axis)

def reference(cell_row, cell_col, cell_width, cell_height, cell_region, cell_offset):
    span_x = jnp.arange(WMAX + 1)
    span_y = jnp.arange(HMAX + 1)
    x_intersect = intersect(span_x[None, :].astype(jnp.float32), cell_offset[0][:, None], cell_width.astype(jnp.float32)[:, None])
    y_intersect = intersect(span_y[None, :].astype(jnp.float32), cell_offset[1][:, None], cell_height.astype(jnp.float32)[:, None])
    weight = y_intersect.astype(jnp.float32)[:, :, None] * x_intersect.astype(jnp.float32)[:, None, :]
    row_index = jnp.broadcast_to(cell_row[:, None, None] + span_y[None, :, None], weight.shape)
    col_index = jnp.broadcast_to(cell_col[:, None, None] + span_x[None, None, :], weight.shape)
    region_index = jnp.broadcast_to(cell_region[:, None, None], weight.shape)
    density = jnp.zeros((REGIONS, M, M), jnp.float32).at[region_index, row_index, col_index].add(weight)
    overflow = jnp.sum(jnp.maximum(density - 1.0, 0.0)) / jnp.sum(density)
    spectrum = dct_forward(dct_forward(density, 2), 1)
    freq_axis = jnp.arange(M).astype(jnp.float32)
    p_grid = freq_axis[:, None]
    q_grid = freq_axis[None, :]
    anchor = jnp.arange(M)[:, None] + jnp.arange(M)[None, :] == 0
    step_size = jnp.pi / M
    squared = p_grid * p_grid + q_grid * q_grid
    potential_hat = jnp.where(anchor, 0.0, spectrum / (step_size * step_size * jnp.where(anchor, 1.0, squared)))
    field_x = dct_inverse(dct_inverse(potential_hat * (step_size * q_grid), 2, True), 1, False)
    field_y = dct_inverse(dct_inverse(potential_hat * (step_size * p_grid), 2, False), 1, True)
    potential = dct_inverse(dct_inverse(potential_hat, 2, False), 1, False)
    energy = jnp.sum(density * potential) / (M * M)
    rounded_x = lax.optimization_barrier(field_x.astype(jnp.bfloat16)).astype(jnp.float32)
    rounded_y = lax.optimization_barrier(field_y.astype(jnp.bfloat16)).astype(jnp.float32)
    force_x = lax.optimization_barrier(jnp.sum(weight * rounded_x[region_index, row_index, col_index], axis=(1, 2)))
    force_y = lax.optimization_barrier(jnp.sum(weight * rounded_y[region_index, row_index, col_index], axis=(1, 2)))
    return (field_x, field_y, jnp.stack([force_x, force_y]), energy, overflow)
```

```python
import functools
import math

import jax
import jax.numpy as jnp
import numpy as np
from jax import lax
from jax.experimental import pallas as pl
from jax.experimental.pallas import tpu as pltpu
from jax.sharding import PartitionSpec as P

M = 2048
REGIONS = 4
SEND_SCALE = 0.125


def shifted(value, axis, steps):
    count = lax.axis_size(axis)
    first, last = (max(0, -steps), min(count, count - steps))
    return lax.ppermute(value, axis, [(source, source + steps) for source in range(first, last)])


def intersect(offset_bins, fraction, extent):
    high_edge = jnp.minimum(offset_bins + 1.0, fraction + extent)
    low_edge = jnp.maximum(offset_bins, fraction)
    return jnp.maximum(high_edge - low_edge, 0.0).astype(jnp.bfloat16)


def basis_tables(length):
    inner = 32
    outer = length // 2 // inner
    position = 2 * lax.iota(jnp.int32, length) + 1

    def small(freq):
        phase = freq[..., None] * position % (4 * length)
        angle = phase.astype(jnp.float32) * (math.pi / (2.0 * length))
        return jnp.cos(angle), jnp.sin(angle)

    coarse_cos, coarse_sin = small(2 * inner * lax.iota(jnp.int32, outer))
    parity = lax.iota(jnp.int32, 2)[:, None]
    fine_cos, fine_sin = small(2 * lax.iota(jnp.int32, inner)[None, :] + parity)
    coarse_cos, coarse_sin, fine_cos, fine_sin = lax.optimization_barrier(
        (coarse_cos, coarse_sin, fine_cos, fine_sin)
    )
    def build(left_a, right_a, left_b, right_b, sign):
        step_rows = min(4, outer) * inner

        def kernel(la, ra, lb, rb, out):
            step = pl.program_id(1)
            for part in range(step_rows // inner):
                at = pl.ds(step * (step_rows // inner) + part, 1)
                value = la[at, :] * ra[0] + sign * (lb[at, :] * rb[0])
                value = value * math.sqrt(2.0 / length)
                if part == 0:
                    first = (pl.program_id(0) == 0) & (step == 0)
                    here = lax.broadcasted_iota(jnp.int32, (inner, length), 0) == 0
                    value = jnp.where(first & here, value * math.sqrt(0.5), value)
                out[pl.ds(part * inner, inner), :] = value

        small_spec = pl.BlockSpec((outer, length), lambda p, i: (0, 0))
        fine_spec = pl.BlockSpec((1, inner, length), lambda p, i: (p, 0, 0))
        steps = outer * inner // step_rows
        return pl.pallas_call(
            kernel,
            out_shape=jax.ShapeDtypeStruct((length, length), jnp.float32),
            grid=(2, steps),
            in_specs=[small_spec, fine_spec, small_spec, fine_spec],
            out_specs=pl.BlockSpec((step_rows, length), lambda p, i: (p * steps + i, 0)),
            cost_estimate=pl.CostEstimate(
                flops=4 * length * length, bytes_accessed=4 * length * length, transcendentals=0
            ),
        )(left_a, right_a, left_b, right_b)

    cosine = build(coarse_cos, fine_cos, coarse_sin, fine_sin, -1.0)
    sine = build(coarse_sin, fine_cos, coarse_cos, fine_sin, 1.0)
    return cosine, sine


def frequency_order(index, length):
    half = length // 2
    return jnp.where(index < half, 2 * index, 2 * (index - half) + 1)


def matmul(left, right, contract):
    return lax.dot_general(
        left,
        right,
        (contract, ((), ())),
        precision=lax.Precision.HIGH,
        preferred_element_type=jnp.float32,
    )


def body(cell_row, cell_col, cell_width, cell_height, cell_region, cell_offset):
    slab_count = lax.axis_size("slab")
    cell_count = lax.axis_size("cell")
    slab_index = lax.axis_index("slab")
    cell_index = lax.axis_index("cell")
    device_count = slab_count * cell_count
    length = M
    regions = REGIONS
    own_regions = regions // cell_count
    rows = length // device_count
    width = length // slab_count
    cells = cell_row.shape[0]
    base_row = (slab_index * cell_count + cell_index) * rows
    everyone = ("slab", "cell")
    cosine, sine = basis_tables(length)

    table = jnp.concatenate(
        [jnp.stack([cell_row, cell_col, cell_width, cell_height, cell_region]).astype(jnp.float32), cell_offset]
    )
    slab_cells = lax.all_gather(table, "cell", axis=1, tiled=True)
    below = shifted(slab_cells, "slab", 1)
    seen = jnp.concatenate([slab_cells, below], axis=1)
    row, col, wide, high, region, off_x, off_y = [seen[i][:, None] for i in range(7)]
    natural = lax.iota(jnp.float32, length)[None, :]
    x_intersect = intersect(natural - col, off_x, wide)
    y_bins = base_row.astype(jnp.float32) + lax.iota(jnp.float32, rows)[None, :] - row
    y_intersect = intersect(y_bins, off_y, high)
    region_hot = region == lax.iota(jnp.float32, regions)[None, :]
    y_region = jnp.where(region_hot[:, :, None], y_intersect[:, None, :], jnp.bfloat16(0)).reshape(
        seen.shape[1], regions * rows
    )
    density = lax.dot_general(
        y_region, x_intersect, (((0,), (0,)), ((), ())), preferred_element_type=jnp.float32
    )
    excess_local = jnp.sum(jnp.maximum(density - 1.0, 0.0))
    area_local = jnp.sum(density)

    by_freq_x = matmul(density, cosine, ((1,), (1,)))
    outgoing = by_freq_x.reshape(cell_count, own_regions, rows, slab_count, width)
    outgoing = outgoing.astype(jnp.float16)
    outgoing = outgoing.transpose(3, 0, 2, 1, 4).reshape(device_count, rows, own_regions * width)
    crossed = lax.all_to_all(outgoing, everyone, split_axis=0, concat_axis=0, tiled=True)
    crossed, sine = lax.optimization_barrier((crossed, sine))
    crossed = crossed.reshape(length, own_regions * width).astype(jnp.float32)
    spectrum = matmul(crossed, cosine, ((0,), (1,)))

    ky_int = frequency_order(lax.iota(jnp.int32, length), length)[None, :]
    kx_int = frequency_order(slab_index * width + lax.iota(jnp.int32, width), length)
    kx_int = jnp.tile(kx_int, own_regions)[:, None]
    kx, ky = kx_int.astype(jnp.float32), ky_int.astype(jnp.float32)
    at_anchor = kx_int + ky_int == 0
    step_size = math.pi / length
    squared = kx * kx + ky * ky
    potential_hat = jnp.where(
        at_anchor, 0.0, spectrum / (step_size * step_size * jnp.where(at_anchor, 1.0, squared))
    )
    energy_local = jnp.sum(spectrum * potential_hat) / (length * length)
    along_x = matmul(potential_hat * (step_size * kx * SEND_SCALE), cosine, ((1,), (0,)))
    along_y = matmul(potential_hat * (step_size * ky * SEND_SCALE), sine, ((1,), (0,)))

    def back(along):
        blocks = along.astype(jnp.float16).T.reshape(device_count, rows, own_regions * width)
        home = lax.all_to_all(blocks, everyone, split_axis=0, concat_axis=0, tiled=True)
        home = home.reshape(slab_count, cell_count, rows, own_regions, width)
        home = home.transpose(1, 3, 2, 0, 4).reshape(regions * rows, length)
        return home.astype(jnp.float32) * (1.0 / SEND_SCALE)

    home_x = back(along_x)
    home_y = back(along_y)
    sums = jnp.stack([excess_local, area_local, energy_local])
    sums, home_y = lax.optimization_barrier((sums, home_y))
    sums = jnp.broadcast_to(sums, (device_count, 3))
    sums = lax.all_to_all(sums, everyone, split_axis=0, concat_axis=0, tiled=True)
    field_x = matmul(home_x, sine, ((1,), (0,)))
    field_y = matmul(home_y, cosine, ((1,), (0,)))

    def pushed(field):
        sampled = lax.dot_general(
            x_intersect,
            field.astype(jnp.bfloat16),
            (((1,), (1,)), ((), ())),
            preferred_element_type=jnp.float32,
        )
        return jnp.sum(sampled * y_region.astype(jnp.float32), axis=1)

    partial = jnp.stack([pushed(field_x), pushed(field_y)])
    here, beneath = partial[:, : cells * cell_count], partial[:, cells * cell_count :]
    here = here + shifted(beneath, "slab", -1)
    here = here.reshape(2, cell_count, cells).transpose(1, 0, 2)
    cell_force = jnp.sum(lax.all_to_all(here, "cell", split_axis=0, concat_axis=0), axis=0)
    excess, area, energy = jnp.sum(sums, axis=0)
    shape = (regions, rows, length)
    return (field_x.reshape(shape), field_y.reshape(shape), cell_force, energy, excess / area)


INNER = 32
FINE = 48
LANES = 128
CODE_TOP = 32000.0


def trig(phase, length):
    angle = (phase % (4 * length)) * (math.pi / (2.0 * length))
    return np.cos(angle).astype(np.float32), np.sin(angle).astype(np.float32)


def small_tables(length):
    half = length // 2
    order = np.concatenate([2 * np.arange(half), 2 * np.arange(half) + 1])[None, :]
    coarse = np.arange(length // INNER)[:, None] * (2 * INNER)
    fine = 2 * np.arange(FINE)[:, None] + 1
    position = 2 * np.arange(half)[None, :] + 1
    freq_coarse = np.arange(half // INNER)[:, None] * (2 * INNER)
    freq_fine = (np.arange(2)[:, None, None] + 2 * np.arange(INNER)[None, :, None]) * position[None]
    return (
        trig(coarse * order, length)
        + trig(fine * order, length)
        + trig(freq_coarse * position, length)
        + trig(freq_fine, length)
    )


def split(value):
    high = value.astype(jnp.bfloat16)
    return high, (value - high.astype(jnp.float32)).astype(jnp.bfloat16)


def dot(left, right, contract=((1,), (0,))):
    return lax.dot_general(left, right, (contract, ((), ())), preferred_element_type=jnp.float32)


def overlap(steps, fraction, extent):
    high_edge = jnp.minimum(steps + 1.0, fraction + extent)
    return jnp.maximum(high_edge - jnp.maximum(steps, fraction), 0.0)


def row_iota(rows, columns):
    return lax.broadcasted_iota(jnp.int32, (rows, columns), 0).astype(jnp.float32)


def fold_rows(value):
    return jnp.sum(value.reshape(value.shape[0] // 8, 8, value.shape[1]), axis=0)


def fused_kernel(
    slab_count, length, cells, regions,
    table, ccos, csin, fcos, fsin, gcos, gsin, hcos, hsin,
    field_x, field_y, force, scalars,
    cells_all, xch, xcl, ych, ycl, ysh, ysl, draw, foh, fol, hxh, hxl, hyh, hyl,
    send_buf, send_scale, recv_buf, recv_scale, rounded, xf, xg, carry, yown, ybelow,
    energy_acc, excess_acc, area_acc, scal_out, scal_in, part_own, part_below, part_sib, part_up,
    cell_send, cell_recv, data_send, data_recv, scale_send, scale_recv,
    scal_send, scal_recv, part_send, part_recv,
):
    half = length // 2
    halves = slab_count // 2
    group = slab_count
    slab_rows = length // slab_count
    rows = slab_rows // 2
    both = 2 * cells
    device_count = 2 * slab_count
    slab = lax.axis_index("slab")
    core = lax.axis_index("cell")
    me = slab * 2 + core
    side = slab // halves
    spot = (slab % halves) * 2 + core
    f32, bf16 = jnp.float32, jnp.bfloat16

    def to(index):
        return (index // 2, index % 2)

    def cell_copy(step):
        return pltpu.make_async_remote_copy(
            src_ref=table, dst_ref=cells_all.at[me], send_sem=cell_send.at[step],
            recv_sem=cell_recv.at[me], device_id=to((me + step) % device_count),
            device_id_type=pl.DeviceIdType.MESH,
        )

    def cell_arrival(source):
        return pltpu.make_async_remote_copy(
            src_ref=table, dst_ref=cells_all.at[source], send_sem=cell_send.at[0],
            recv_sem=cell_recv.at[source], device_id=to((me + 1) % device_count),
            device_id_type=pl.DeviceIdType.MESH,
        )

    barrier = pltpu.get_barrier_semaphore()

    def greet(step, _):
        pl.semaphore_signal(
            barrier, inc=1, device_id=to((me + step) % device_count), device_id_type=pl.DeviceIdType.MESH
        )
        return 0

    lax.fori_loop(1, device_count, greet, 0)
    pl.semaphore_wait(barrier, device_count - 1)

    def send_cells(step, _):
        cell_copy(step).start()
        return 0

    lax.fori_loop(1, device_count, send_cells, 0)
    cells_all[me] = table[...]

    def rotate(cos_a, sin_a, cos_b, sin_b):
        return cos_a * cos_b - sin_a * sin_b, sin_a * cos_b + cos_a * sin_b

    def build_y(step, _):
        at = pl.ds(pl.multiple_of(step * INNER, INNER), INNER)
        row = pl.ds(side * (half // INNER) + step, 1)
        for parity in range(2):
            for part in range(half // 256):
                lanes = pl.ds(parity * half + part * 256, 256)
                out = pl.ds(part * 256, 256)
                cosine, sine = rotate(
                    ccos[row, lanes], csin[row, lanes], fcos[:INNER, lanes], fsin[:INNER, lanes]
                )
                ych[parity, at, out], ycl[parity, at, out] = split(cosine)
                ysh[parity, at, out], ysl[parity, at, out] = split(sine)
        return 0

    def build_x(step, high, low, pick):
        at = pl.ds(pl.multiple_of(step * INNER, INNER), INNER)
        row = pl.ds(step, 1)
        for parity in range(2):
            for part in range(half // 256):
                lanes = pl.ds(part * 256, 256)
                value = rotate(gcos[row, lanes], gsin[row, lanes], hcos[parity, :, lanes], hsin[parity, :, lanes])
                high[parity, at, lanes], low[parity, at, lanes] = split(value[pick])
        return 0

    lax.fori_loop(0, half // INNER, lambda s, c: build_x(s, xch, xcl, 0), 0)
    lax.fori_loop(0, half // INNER, build_y, 0)

    mine = pl.ds(pl.multiple_of(spot * LANES, LANES), LANES)
    coarse_rows = length // INNER
    for index, (fine_ref, coarse_ref) in enumerate(((fcos, ccos), (fsin, csin))):
        into = pl.ds(index * LANES, LANES)
        pad = jnp.zeros((LANES - FINE, LANES), f32)
        value = fine_ref[:, mine]
        high = value.astype(bf16).astype(f32)
        xf[into, :LANES] = jnp.concatenate([high, pad], 0).T.astype(bf16)
        xf[into, LANES:] = jnp.concatenate([value - high, pad], 0).T.astype(bf16)
        value = coarse_ref[:, mine]
        high = value.astype(bf16).astype(f32)
        xg[into, :] = jnp.concatenate([high, value - high], 0).T.astype(bf16)

    def take_cells(step, _):
        cell_arrival((me + step) % device_count).wait_recv()
        return 0

    lax.fori_loop(1, device_count, take_cells, 0)

    def slab_cells(index):
        block = jnp.concatenate([cells_all[2 * index], cells_all[2 * index + 1]], axis=1)
        return [block[i : i + 1, :] for i in range(7)]

    carry[...] = jnp.zeros_like(carry)

    def spread(index, _):
        row, col, wide, high, region, off_x, off_y = slab_cells(index)
        upper = index // halves
        window = jnp.floor(col * (1.0 / INNER))
        local = col - window * INNER
        near = overlap(row_iota(FINE, both) - local, off_x, wide).astype(bf16)
        gap = jnp.zeros((LANES - FINE, both), bf16)
        hot = jnp.where(row_iota(coarse_rows, both) == window, 1.0, 0.0).astype(bf16)
        fine_part = dot(xf[...], jnp.concatenate([near, gap, near, gap], 0))
        coarse_part = dot(xg[...], jnp.concatenate([hot, hot], 0))
        along = fine_part[:LANES] * coarse_part[:LANES] - fine_part[LANES:] * coarse_part[LANES:]
        waves = jnp.concatenate(split(along), 0)
        start = (index * slab_rows).astype(f32)
        flip = upper.astype(f32)
        ladder = row_iota(slab_rows, both)
        place = start + ladder + flip * (slab_rows - 1.0 - 2.0 * ladder)
        tall = overlap(place - row, off_y, high).astype(bf16)
        flip_next = ((index + 1) // halves).astype(f32)
        steps = row_iota(8, both)
        place = start + slab_rows + steps + flip_next * (7.0 - 2.0 * steps)
        above = overlap(place - row, off_y, high)
        masks = [jnp.where(region == g, 1.0, 0.0) for g in range(regions)]
        above = jnp.concatenate([above * mask for mask in masks], 0).astype(bf16)
        stack = jnp.concatenate([tall * mask.astype(bf16) for mask in masks] + [above], 0)
        result = dot(stack, waves, ((1,), (1,)))
        result = result[:, :LANES] + result[:, LANES:]
        tile = index + upper * (2 * halves - 1 - 2 * index)
        base = pl.multiple_of(tile * slab_rows, slab_rows)
        edge = pl.multiple_of(tile * slab_rows + upper * (slab_rows - 8), 8)
        for g in range(regions):
            lanes = pl.ds(g * LANES, LANES)
            draw[upper, pl.ds(base, slab_rows), lanes] = result[g * slab_rows : (g + 1) * slab_rows]
            draw[upper, pl.ds(edge, 8), lanes] += carry[g * 8 : (g + 1) * 8, :]
        carry[...] = result[regions * slab_rows :]
        return 0

    lax.fori_loop(0, slab_count, spread, 0)

    def fold(step, _):
        at = pl.ds(pl.multiple_of(step * 64, 64), 64)
        lower, upper = draw[0, at, :], draw[1, at, :]
        foh[0, at, :], fol[0, at, :] = split(lower + upper)
        foh[1, at, :], fol[1, at, :] = split(lower - upper)
        return 0

    lax.fori_loop(0, half // 64, fold, 0)

    step_size = math.pi / length
    energy_acc[...] = jnp.zeros_like(energy_acc)
    chunk = 256
    kx = 2 * ((spot % halves) * LANES + lax.broadcasted_iota(jnp.int32, (chunk, LANES), 1)) + spot // halves
    kx = kx.astype(f32)

    def transform(step, _):
        parity = step // (half // chunk)
        first = (step % (half // chunk)) * chunk
        at = pl.ds(pl.multiple_of(first, chunk), chunk)
        high, low = xch[parity, at, :], xcl[parity, at, :]
        spectrum = dot(high, foh[parity]) + (dot(high, fol[parity]) + dot(low, foh[parity]))
        ky = (2 * (first + lax.broadcasted_iota(jnp.int32, (chunk, LANES), 0)) + parity).astype(f32)
        squared = kx * kx + ky * ky
        at_anchor = squared == 0.0
        scale = jnp.where(kx == 0.0, 1.0 / length, 2.0 / length) * jnp.where(ky == 0.0, 1.0 / length, 2.0 / length)
        weight = jnp.where(
            at_anchor, 0.0, scale / (step_size * step_size * jnp.where(at_anchor, 1.0, squared))
        )
        weight_x = weight * (step_size * kx)
        weight_y = weight * (step_size * ky)
        energy = energy_acc[...]
        for g in range(regions):
            lanes = pl.ds(g * LANES, LANES)
            part = spectrum[:, g * LANES : (g + 1) * LANES]
            hxh[parity, at, lanes], hxl[parity, at, lanes] = split(part * weight_x)
            hyh[parity, at, lanes], hyl[parity, at, lanes] = split(part * weight_y)
            energy += fold_rows(part * part * weight)
        energy_acc[...] = energy
        return 0

    lax.fori_loop(0, 2 * (half // chunk), transform, 0)

    def data_copy(target, source, place):
        return pltpu.make_async_remote_copy(
            src_ref=send_buf.at[target], dst_ref=recv_buf.at[source], send_sem=data_send.at[target],
            recv_sem=data_recv.at[source], device_id=to(side * group + place), device_id_type=pl.DeviceIdType.MESH,
        )

    def scale_copy(target, source, place):
        return pltpu.make_async_remote_copy(
            src_ref=send_scale.at[target], dst_ref=recv_scale.at[source], send_sem=scale_send.at[target],
            recv_sem=scale_recv.at[source], device_id=to(side * group + place), device_id_type=pl.DeviceIdType.MESH,
        )

    tiles = group // 4

    def inverse(step, _):
        tile = (spot // 4 + step + 1) % tiles
        at = pl.ds(pl.multiple_of(tile * (4 * rows), 4 * rows), 4 * rows)
        for index, (th, tl, vh, vl) in enumerate(((ych, ycl, hxh, hxl), (ysh, ysl, hyh, hyl))):
            value = None
            for parity in range(2):
                high, low = th[parity, at, :], tl[parity, at, :]
                term = dot(high, vh[parity]) + (dot(high, vl[parity]) + dot(low, vh[parity]))
                value = term if value is None else value + term
            for part in range(4):
                block = value[part * rows : (part + 1) * rows]
                top = jnp.maximum(jnp.max(jnp.abs(block), axis=0, keepdims=True), 1e-30)
                code = jnp.round(block * (CODE_TOP / top)).astype(jnp.int32).astype(jnp.int16)
                send_buf[tile * 4 + part, index] = code
                send_scale[tile * 4 + part, pl.ds(index, 1), :] = top * (1.0 / CODE_TOP)
        for part in range(4):
            target = tile * 4 + part

            @pl.when(target != spot)
            def _():
                data_copy(target, spot, target).start()
                scale_copy(target, spot, target).start()

            @pl.when(target == spot)
            def _():
                recv_buf[spot] = send_buf[spot]
                recv_scale[spot] = send_scale[spot]

        return 0

    lax.fori_loop(0, tiles, inverse, 0)

    own = slab_cells(slab)
    under = slab_cells((slab + slab_count - 1) % slab_count)
    start = (slab * slab_rows + core * rows).astype(f32)
    for count, ref, (row, _, _, high, region, _, off_y) in ((rows, yown, own), (8, ybelow, under)):
        reach = overlap(start + row_iota(count, both) - row, off_y, high)
        for g in range(regions):
            ref[pl.ds(g * count, count), :] = jnp.where(region == g, reach, 0.0).astype(bf16)

    def columns(step, _):
        at = pl.ds(pl.multiple_of(step * 64, 64), 64)
        for part in range(2):
            spots = row_iota(64, both) + (step * 64 + part * half).astype(f32)
            for ref, (_, col, wide, _, _, off_x, _) in ((ych, own), (ycl, under)):
                ref[part, at, :] = overlap(spots - col, off_x, wide).astype(bf16)
        return 0

    lax.fori_loop(0, half // 64, columns, 0)
    excess_acc[...] = jnp.zeros_like(excess_acc)
    area_acc[...] = jnp.zeros_like(area_acc)

    def measure(step, _):
        part = step // (half // 256)
        at = pl.ds(pl.multiple_of((step % (half // 256)) * 256, 256), 256)
        density = dot(yown[...], ych[part, at, :], ((1,), (1,)))
        extra = dot(ybelow[...], ycl[part, at, :], ((1,), (1,)))
        excess, area = excess_acc[...], area_acc[...]
        for g in range(regions):
            block = density[g * rows : (g + 1) * rows]
            for piece in (block[:8] + extra[g * 8 : (g + 1) * 8], block[8:]):
                area += fold_rows(piece)
                excess += fold_rows(jnp.maximum(piece - 1.0, 0.0))
        excess_acc[...], area_acc[...] = excess, area
        return 0

    lax.fori_loop(0, length // 256, measure, 0)

    lane = lax.broadcasted_iota(jnp.int32, (8, LANES), 1)
    sums = jnp.where(lane == 0, jnp.sum(excess_acc[...]), 0.0)
    sums = jnp.where(lane == 1, jnp.sum(area_acc[...]), sums)
    sums = jnp.where(lane == 2, jnp.sum(energy_acc[...]) * (0.5 / (length * length)), sums)
    scal_out[...] = sums
    scal_in[me] = sums

    def scal_copy(step, source):
        return pltpu.make_async_remote_copy(
            src_ref=scal_out, dst_ref=scal_in.at[source], send_sem=scal_send.at[step],
            recv_sem=scal_recv.at[source], device_id=to((me + step) % device_count),
            device_id_type=pl.DeviceIdType.MESH,
        )

    def send_sums(step, _):
        scal_copy(step, me).start()
        return 0

    lax.fori_loop(1, device_count, send_sums, 0)
    lax.fori_loop(0, half // INNER, lambda s, c: build_x(s, ysh, ysl, 1), 0)

    def unpack(step, _):
        source = (spot + step) % group

        @pl.when(source != spot)
        def _():
            data_copy(source, source, source).wait_recv()
            scale_copy(source, source, source).wait_recv()

        across = source // 4
        lanes = pl.ds(pl.multiple_of((source % 4) * LANES, LANES), LANES)
        for index in range(2):
            factor = recv_scale[source, pl.ds(index, 1), :]
            value = recv_buf[source, index].astype(jnp.int32).astype(f32) * factor
            for g in range(regions):
                at = pl.ds(pl.multiple_of(across * (regions * rows) + g * rows, rows), rows)
                foh[index, at, lanes], fol[index, at, lanes] = split(value[:, g * LANES : (g + 1) * LANES])
        return 0

    lax.fori_loop(0, group, unpack, 0)

    high_rows = regions * rows
    mirror = LANES - 1 - lax.broadcasted_iota(jnp.int32, (high_rows, LANES), 1)
    wide = 256
    for index, (th, tl, out) in enumerate(((ysh, ysl, field_x), (xch, xcl, field_y))):

        def finish(step, _, index=index, th=th, tl=tl, out=out):
            at = pl.ds(pl.multiple_of(step * wide, wide), wide)
            sums = []
            for parity in range(2):
                total = None
                for block in range(2):
                    pick = pl.ds((parity * 2 + block) * high_rows, high_rows)
                    high, low = foh[index, pick, :], fol[index, pick, :]
                    depth = pl.ds(block * 512, 512)
                    left, right = th[parity, depth, at], tl[parity, depth, at]
                    term = dot(high, left) + (dot(high, right) + dot(low, left))
                    total = term if total is None else total + term
                sums.append(total)
            even, odd = sums
            straight = even + odd
            back = even - odd if index else odd - even
            rounded[index, :, at] = straight.astype(bf16)
            for g in range(regions):
                out[g, :, at] = straight[g * rows : (g + 1) * rows]
            for part in range(wide // LANES):
                tile = jnp.take_along_axis(
                    back[:, part * LANES : (part + 1) * LANES], mirror, axis=1, mode="promise_in_bounds"
                )
                far = pl.ds(pl.multiple_of(length - (part + 1) * LANES - step * wide, LANES), LANES)
                rounded[index, :, far] = tile.astype(bf16)
                for g in range(regions):
                    out[g, :, far] = tile[g * rows : (g + 1) * rows]
            return 0

        lax.fori_loop(0, half // wide, finish, 0)

    for index, out in enumerate((field_x, field_y)):
        low_rows = jnp.concatenate([out[g, :8, :] for g in range(regions)], 0).astype(bf16)
        total = dot(rounded[index, :, :half], ych[0]) + dot(rounded[index, :, half:], ych[1])
        extra = dot(low_rows[:, :half], ycl[0]) + dot(low_rows[:, half:], ycl[1])
        total = jnp.sum(total * yown[...].astype(f32), axis=0, keepdims=True)
        extra = jnp.sum(extra * ybelow[...].astype(f32), axis=0, keepdims=True)
        for part in range(2):
            part_own[part, pl.ds(index, 1), :] = total[:, part * cells : (part + 1) * cells]
            part_below[part, pl.ds(index, 1), :] = extra[:, part * cells : (part + 1) * cells]

    def sibling_copy():
        return pltpu.make_async_remote_copy(
            src_ref=part_own.at[1 - core], dst_ref=part_sib, send_sem=part_send.at[0],
            recv_sem=part_recv.at[0], device_id=(slab, 1 - core), device_id_type=pl.DeviceIdType.MESH,
        )

    def down_copy(part):
        return pltpu.make_async_remote_copy(
            src_ref=part_below.at[part], dst_ref=part_up, send_sem=part_send.at[1 + part],
            recv_sem=part_recv.at[1], device_id=(lax.max(slab - 1, 0), part),
            device_id_type=pl.DeviceIdType.MESH,
        )

    sibling_copy().start()

    @pl.when((core == 0) & (slab > 0))
    def _():
        down_copy(0).start()
        down_copy(1).start()

    def take_sums(step, _):
        scal_copy(step, (me + step) % device_count).wait_recv()
        return 0

    lax.fori_loop(1, device_count, take_sums, 0)
    total = scal_in[0]
    for source in range(1, device_count):
        total += scal_in[source]
    scalars[...] = total
    sibling_copy().wait_recv()
    force[...] = (part_own[core] + part_sib[...])[:2]

    @pl.when(slab < slab_count - 1)
    def _():
        down_copy(0).wait_recv()
        force[...] += part_up[:2, :]

    def drain(step, _):
        cell_copy(step).wait_send()
        scal_copy(step, me).wait_send()
        return 0

    lax.fori_loop(1, device_count, drain, 0)

    def drain_data(step, _):
        target = (spot + step) % group
        data_copy(target, spot, target).wait_send()
        scale_copy(target, spot, target).wait_send()
        return 0

    lax.fori_loop(1, group, drain_data, 0)
    sibling_copy().wait_send()

    @pl.when((core == 0) & (slab > 0))
    def _():
        down_copy(0).wait_send()
        down_copy(1).wait_send()


def fused_body(cell_row, cell_col, cell_width, cell_height, cell_region, cell_offset):
    slab_count = lax.axis_size("slab")
    length, regions = M, REGIONS
    cells = cell_row.shape[0]
    half, group = length // 2, slab_count
    device_count = 2 * slab_count
    rows = length // device_count
    f32, bf16 = jnp.float32, jnp.bfloat16
    table = jnp.concatenate(
        [
            jnp.stack([cell_row, cell_col, cell_width, cell_height, cell_region]).astype(f32),
            cell_offset,
            jnp.zeros((1, cells), f32),
        ]
    )
    consts = [jnp.asarray(t) for t in small_tables(length)]
    vmem = pltpu.VMEM
    basis = vmem((2, half, half), bf16)
    panel = vmem((2, half, regions * LANES), bf16)
    sems = pltpu.SemaphoreType.DMA
    scratch = (
        [vmem((device_count, 8, cells), f32)]
        + [basis] * 6
        + [vmem((2, half, regions * LANES), f32)]
        + [panel] * 6
        + [
            vmem((group, 2, rows, regions * LANES), jnp.int16),
            vmem((group, 2, regions * LANES), f32),
            vmem((group, 2, rows, regions * LANES), jnp.int16),
            vmem((group, 2, regions * LANES), f32),
            vmem((2, regions * rows, length), bf16),
            vmem((2 * LANES, 2 * LANES), bf16),
            vmem((2 * LANES, 2 * (length // INNER)), bf16),
            vmem((8 * regions, LANES), f32),
            vmem((regions * rows, 2 * cells), bf16),
            vmem((8 * regions, 2 * cells), bf16),
            vmem((8, LANES), f32),
            vmem((8, 256), f32),
            vmem((8, 256), f32),
            vmem((8, LANES), f32),
            vmem((device_count, 8, LANES), f32),
            vmem((2, 8, cells), f32),
            vmem((2, 8, cells), f32),
            vmem((8, cells), f32),
            vmem((8, cells), f32),
            sems((device_count,)),
            sems((device_count,)),
            sems((group,)),
            sems((group,)),
            sems((group,)),
            sems((group,)),
            sems((device_count,)),
            sems((device_count,)),
            sems((3,)),
            sems((2,)),
        ]
    )
    whole = pl.BlockSpec(memory_space=vmem)
    field = jax.ShapeDtypeStruct((regions, rows, length), f32)
    field_x, field_y, force, scalars = pl.pallas_call(
        functools.partial(fused_kernel, slab_count, length, cells, regions),
        out_shape=(
            field,
            field,
            jax.ShapeDtypeStruct((2, cells), f32),
            jax.ShapeDtypeStruct((8, LANES), f32),
        ),
        in_specs=[whole] * (1 + len(consts)),
        out_specs=(whole,) * 4,
        scratch_shapes=scratch,
        compiler_params=pltpu.CompilerParams(
            collective_id=0, has_side_effects=True, vmem_limit_bytes=67043328
        ),
    )(table, *consts)
    return field_x, field_y, force, scalars[0, 2], scalars[0, 0] / scalars[0, 1]


def fits(mesh):
    slab_count = mesh.shape["slab"]
    return mesh.shape["cell"] == 2 and slab_count % 8 == 0 and M == slab_count * LANES


def solution(mesh):
    return jax.shard_map(
        fused_body if fits(mesh) else body,
        mesh=mesh,
        in_specs=(
            P(("slab", "cell")),
            P(("slab", "cell")),
            P(("slab", "cell")),
            P(("slab", "cell")),
            P(("slab", "cell")),
            P(None, ("slab", "cell")),
        ),
        out_specs=(
            P(None, ("slab", "cell"), None),
            P(None, ("slab", "cell"), None),
            P(None, ("slab", "cell")),
            P(),
            P(),
        ),
        check_vma=False,
    )
```

```python
import functools
import math

import jax
import jax.numpy as jnp
import numpy as np
from jax import lax
from jax.experimental import pallas as pl
from jax.experimental.pallas import tpu as pltpu
from jax.sharding import PartitionSpec as P

M = 2048
REGIONS = 4
SEND_SCALE = 0.125


def shifted(value, axis, steps):
    count = lax.axis_size(axis)
    first, last = (max(0, -steps), min(count, count - steps))
    return lax.ppermute(value, axis, [(source, source + steps) for source in range(first, last)])


def intersect(offset_bins, fraction, extent):
    high_edge = jnp.minimum(offset_bins + 1.0, fraction + extent)
    low_edge = jnp.maximum(offset_bins, fraction)
    return jnp.maximum(high_edge - low_edge, 0.0).astype(jnp.bfloat16)


def basis_tables(length):
    inner = 32
    outer = length // 2 // inner
    position = 2 * lax.iota(jnp.int32, length) + 1

    def small(freq):
        phase = freq[..., None] * position % (4 * length)
        angle = phase.astype(jnp.float32) * (math.pi / (2.0 * length))
        return jnp.cos(angle), jnp.sin(angle)

    coarse_cos, coarse_sin = small(2 * inner * lax.iota(jnp.int32, outer))
    parity = lax.iota(jnp.int32, 2)[:, None]
    fine_cos, fine_sin = small(2 * lax.iota(jnp.int32, inner)[None, :] + parity)
    coarse_cos, coarse_sin, fine_cos, fine_sin = lax.optimization_barrier(
        (coarse_cos, coarse_sin, fine_cos, fine_sin)
    )
    def build(left_a, right_a, left_b, right_b, sign):
        step_rows = min(4, outer) * inner

        def kernel(la, ra, lb, rb, out):
            step = pl.program_id(1)
            for part in range(step_rows // inner):
                at = pl.ds(step * (step_rows // inner) + part, 1)
                value = la[at, :] * ra[0] + sign * (lb[at, :] * rb[0])
                value = value * math.sqrt(2.0 / length)
                if part == 0:
                    first = (pl.program_id(0) == 0) & (step == 0)
                    here = lax.broadcasted_iota(jnp.int32, (inner, length), 0) == 0
                    value = jnp.where(first & here, value * math.sqrt(0.5), value)
                out[pl.ds(part * inner, inner), :] = value

        small_spec = pl.BlockSpec((outer, length), lambda p, i: (0, 0))
        fine_spec = pl.BlockSpec((1, inner, length), lambda p, i: (p, 0, 0))
        steps = outer * inner // step_rows
        return pl.pallas_call(
            kernel,
            out_shape=jax.ShapeDtypeStruct((length, length), jnp.float32),
            grid=(2, steps),
            in_specs=[small_spec, fine_spec, small_spec, fine_spec],
            out_specs=pl.BlockSpec((step_rows, length), lambda p, i: (p * steps + i, 0)),
            cost_estimate=pl.CostEstimate(
                flops=4 * length * length, bytes_accessed=4 * length * length, transcendentals=0
            ),
        )(left_a, right_a, left_b, right_b)

    cosine = build(coarse_cos, fine_cos, coarse_sin, fine_sin, -1.0)
    sine = build(coarse_sin, fine_cos, coarse_cos, fine_sin, 1.0)
    return cosine, sine


def frequency_order(index, length):
    half = length // 2
    return jnp.where(index < half, 2 * index, 2 * (index - half) + 1)


def matmul(left, right, contract):
    return lax.dot_general(
        left,
        right,
        (contract, ((), ())),
        precision=lax.Precision.HIGH,
        preferred_element_type=jnp.float32,
    )


def body(cell_row, cell_col, cell_width, cell_height, cell_region, cell_offset):
    slab_count = lax.axis_size("slab")
    cell_count = lax.axis_size("cell")
    slab_index = lax.axis_index("slab")
    cell_index = lax.axis_index("cell")
    device_count = slab_count * cell_count
    length = M
    regions = REGIONS
    own_regions = regions // cell_count
    rows = length // device_count
    width = length // slab_count
    cells = cell_row.shape[0]
    base_row = (slab_index * cell_count + cell_index) * rows
    everyone = ("slab", "cell")
    cosine, sine = basis_tables(length)

    table = jnp.concatenate(
        [jnp.stack([cell_row, cell_col, cell_width, cell_height, cell_region]).astype(jnp.float32), cell_offset]
    )
    slab_cells = lax.all_gather(table, "cell", axis=1, tiled=True)
    below = shifted(slab_cells, "slab", 1)
    seen = jnp.concatenate([slab_cells, below], axis=1)
    row, col, wide, high, region, off_x, off_y = [seen[i][:, None] for i in range(7)]
    natural = lax.iota(jnp.float32, length)[None, :]
    x_intersect = intersect(natural - col, off_x, wide)
    y_bins = base_row.astype(jnp.float32) + lax.iota(jnp.float32, rows)[None, :] - row
    y_intersect = intersect(y_bins, off_y, high)
    region_hot = region == lax.iota(jnp.float32, regions)[None, :]
    y_region = jnp.where(region_hot[:, :, None], y_intersect[:, None, :], jnp.bfloat16(0)).reshape(
        seen.shape[1], regions * rows
    )
    density = lax.dot_general(
        y_region, x_intersect, (((0,), (0,)), ((), ())), preferred_element_type=jnp.float32
    )
    excess_local = jnp.sum(jnp.maximum(density - 1.0, 0.0))
    area_local = jnp.sum(density)

    by_freq_x = matmul(density, cosine, ((1,), (1,)))
    outgoing = by_freq_x.reshape(cell_count, own_regions, rows, slab_count, width)
    outgoing = outgoing.astype(jnp.float16)
    outgoing = outgoing.transpose(3, 0, 2, 1, 4).reshape(device_count, rows, own_regions * width)
    crossed = lax.all_to_all(outgoing, everyone, split_axis=0, concat_axis=0, tiled=True)
    crossed, sine = lax.optimization_barrier((crossed, sine))
    crossed = crossed.reshape(length, own_regions * width).astype(jnp.float32)
    spectrum = matmul(crossed, cosine, ((0,), (1,)))

    ky_int = frequency_order(lax.iota(jnp.int32, length), length)[None, :]
    kx_int = frequency_order(slab_index * width + lax.iota(jnp.int32, width), length)
    kx_int = jnp.tile(kx_int, own_regions)[:, None]
    kx, ky = kx_int.astype(jnp.float32), ky_int.astype(jnp.float32)
    at_anchor = kx_int + ky_int == 0
    step_size = math.pi / length
    squared = kx * kx + ky * ky
    potential_hat = jnp.where(
        at_anchor, 0.0, spectrum / (step_size * step_size * jnp.where(at_anchor, 1.0, squared))
    )
    energy_local = jnp.sum(spectrum * potential_hat) / (length * length)
    along_x = matmul(potential_hat * (step_size * kx * SEND_SCALE), cosine, ((1,), (0,)))
    along_y = matmul(potential_hat * (step_size * ky * SEND_SCALE), sine, ((1,), (0,)))

    def back(along):
        blocks = along.astype(jnp.float16).T.reshape(device_count, rows, own_regions * width)
        home = lax.all_to_all(blocks, everyone, split_axis=0, concat_axis=0, tiled=True)
        home = home.reshape(slab_count, cell_count, rows, own_regions, width)
        home = home.transpose(1, 3, 2, 0, 4).reshape(regions * rows, length)
        return home.astype(jnp.float32) * (1.0 / SEND_SCALE)

    home_x = back(along_x)
    home_y = back(along_y)
    sums = jnp.stack([excess_local, area_local, energy_local])
    sums, home_y = lax.optimization_barrier((sums, home_y))
    sums = jnp.broadcast_to(sums, (device_count, 3))
    sums = lax.all_to_all(sums, everyone, split_axis=0, concat_axis=0, tiled=True)
    field_x = matmul(home_x, sine, ((1,), (0,)))
    field_y = matmul(home_y, cosine, ((1,), (0,)))

    def pushed(field):
        sampled = lax.dot_general(
            x_intersect,
            field.astype(jnp.bfloat16),
            (((1,), (1,)), ((), ())),
            preferred_element_type=jnp.float32,
        )
        return jnp.sum(sampled * y_region.astype(jnp.float32), axis=1)

    partial = jnp.stack([pushed(field_x), pushed(field_y)])
    here, beneath = partial[:, : cells * cell_count], partial[:, cells * cell_count :]
    here = here + shifted(beneath, "slab", -1)
    here = here.reshape(2, cell_count, cells).transpose(1, 0, 2)
    cell_force = jnp.sum(lax.all_to_all(here, "cell", split_axis=0, concat_axis=0), axis=0)
    excess, area, energy = jnp.sum(sums, axis=0)
    shape = (regions, rows, length)
    return (field_x.reshape(shape), field_y.reshape(shape), cell_force, energy, excess / area)


INNER = 32
FINE = 48
LANES = 128
CODE_TOP = 32000.0


def trig(phase, length):
    angle = (phase % (4 * length)) * (math.pi / (2.0 * length))
    return np.cos(angle).astype(np.float32), np.sin(angle).astype(np.float32)


def small_tables(length):
    half = length // 2
    order = np.concatenate([2 * np.arange(half), 2 * np.arange(half) + 1])[None, :]
    coarse = np.arange(length // INNER)[:, None] * (2 * INNER)
    fine = 2 * np.arange(FINE)[:, None] + 1
    position = 2 * np.arange(half)[None, :] + 1
    freq_coarse = np.arange(half // INNER)[:, None] * (2 * INNER)
    freq_fine = (np.arange(2)[:, None, None] + 2 * np.arange(INNER)[None, :, None]) * position[None]
    return (
        trig(coarse * order, length)
        + trig(fine * order, length)
        + trig(freq_coarse * position, length)
        + trig(freq_fine, length)
    )


def split(value):
    high = value.astype(jnp.bfloat16)
    return high, (value - high.astype(jnp.float32)).astype(jnp.bfloat16)


def dot(left, right, contract=((1,), (0,))):
    return lax.dot_general(left, right, (contract, ((), ())), preferred_element_type=jnp.float32)


def overlap(steps, fraction, extent):
    high_edge = jnp.minimum(steps + 1.0, fraction + extent)
    return jnp.maximum(high_edge - jnp.maximum(steps, fraction), 0.0)


def row_iota(rows, columns):
    return lax.broadcasted_iota(jnp.int32, (rows, columns), 0).astype(jnp.float32)


def fold_rows(value):
    return jnp.sum(value.reshape(value.shape[0] // 8, 8, value.shape[1]), axis=0)


def fused_kernel(
    slab_count, length, cells, regions,
    cell_row, cell_col, cell_width, cell_height, cell_region, cell_offset, ccos, csin, fcos, fsin, gcos, gsin, hcos, hsin,
    out_x, out_y, force, scalars,
    table, field_x, field_y, cells_all, xch, xcl, ych, ycl, ysh, ysl, draw, foh, fol, hxh, hxl, hyh, hyl,
    send_buf, send_scale, recv_buf, recv_scale, rounded, xf, xg, carry, yown, ybelow,
    energy_acc, excess_acc, area_acc, scal_out, scal_in, part_own, part_below, part_sib, part_up,
    cell_send, cell_recv, data_send, data_recv, scale_send, scale_recv,
    scal_send, scal_recv, part_send, part_recv, out_sem,
):
    half = length // 2
    halves = slab_count // 2
    group = slab_count
    slab_rows = length // slab_count
    rows = slab_rows // 2
    both = 2 * cells
    device_count = 2 * slab_count
    slab = lax.axis_index("slab")
    core = lax.axis_index("cell")
    me = slab * 2 + core
    side = slab // halves
    spot = (slab % halves) * 2 + core
    f32, bf16 = jnp.float32, jnp.bfloat16

    def to(index):
        return (index // 2, index % 2)

    def neighbour(step):
        return ((slab + step // 2) % slab_count, (core + step) % 2)

    def cell_copy(step):
        return pltpu.make_async_remote_copy(
            src_ref=table, dst_ref=cells_all.at[me], send_sem=cell_send.at[step],
            recv_sem=cell_recv.at[me], device_id=neighbour(step),
            device_id_type=pl.DeviceIdType.MESH,
        )

    def cell_arrival(source):
        return pltpu.make_async_remote_copy(
            src_ref=table, dst_ref=cells_all.at[source], send_sem=cell_send.at[0],
            recv_sem=cell_recv.at[source], device_id=to((me + 1) % device_count),
            device_id_type=pl.DeviceIdType.MESH,
        )

    barrier = pltpu.get_barrier_semaphore()

    def greet(step, _):
        pl.semaphore_signal(
            barrier, inc=1, device_id=to((me + step) % device_count), device_id_type=pl.DeviceIdType.MESH
        )
        return 0

    lax.fori_loop(1, device_count, greet, 0)
    for index, ref in enumerate((cell_row, cell_col, cell_width, cell_height, cell_region)):
        table[pl.ds(index, 1), :] = ref[...].reshape(1, cells).astype(f32)
    table[5:7, :] = cell_offset[...]
    table[7:8, :] = jnp.zeros((1, cells), f32)
    pl.semaphore_wait(barrier, device_count - 1)

    def send_cells(step, _):
        cell_copy(step).start()
        return 0

    lax.fori_loop(1, device_count, send_cells, 0)
    cells_all[me] = table[...]

    def rotate(cos_a, sin_a, cos_b, sin_b):
        return cos_a * cos_b - sin_a * sin_b, sin_a * cos_b + cos_a * sin_b

    def build_y(step, _):
        at = pl.ds(pl.multiple_of(step * INNER, INNER), INNER)
        row = pl.ds(side * (half // INNER) + step, 1)
        for parity in range(2):
            for part in range(half // 256):
                lanes = pl.ds(parity * half + part * 256, 256)
                out = pl.ds(part * 256, 256)
                cosine, sine = rotate(
                    ccos[row, lanes], csin[row, lanes], fcos[:INNER, lanes], fsin[:INNER, lanes]
                )
                ych[parity, at, out], ycl[parity, at, out] = split(cosine)
                ysh[parity, at, out], ysl[parity, at, out] = split(sine)
        return 0

    def build_x(step, high, low, pick):
        at = pl.ds(pl.multiple_of(step * INNER, INNER), INNER)
        row = pl.ds(step, 1)
        for parity in range(2):
            for part in range(half // 256):
                lanes = pl.ds(part * 256, 256)
                value = rotate(gcos[row, lanes], gsin[row, lanes], hcos[parity, :, lanes], hsin[parity, :, lanes])
                high[parity, at, lanes], low[parity, at, lanes] = split(value[pick])
        return 0

    lax.fori_loop(0, half // INNER, lambda s, c: build_x(s, xch, xcl, 0), 0)
    lax.fori_loop(0, half // INNER, build_y, 0)

    mine = pl.ds(pl.multiple_of(spot * LANES, LANES), LANES)
    coarse_rows = length // INNER
    for index, (fine_ref, coarse_ref) in enumerate(((fcos, ccos), (fsin, csin))):
        into = pl.ds(index * LANES, LANES)
        pad = jnp.zeros((LANES - FINE, LANES), f32)
        value = fine_ref[:, mine]
        high = value.astype(bf16).astype(f32)
        xf[into, :LANES] = jnp.concatenate([high, pad], 0).T.astype(bf16)
        xf[into, LANES:] = jnp.concatenate([value - high, pad], 0).T.astype(bf16)
        value = coarse_ref[:, mine]
        high = value.astype(bf16).astype(f32)
        xg[into, :] = jnp.concatenate([high, value - high], 0).T.astype(bf16)

    def slab_cells(index):
        block = jnp.concatenate([cells_all[2 * index], cells_all[2 * index + 1]], axis=1)
        return [block[i : i + 1, :] for i in range(7)]

    def spread(step, _):
        index = (slab + slab_count - step) % slab_count
        for part in range(2):

            @pl.when(2 * index + part != me)
            def _():
                cell_arrival(2 * index + part).wait_recv()

        row, col, wide, high, region, off_x, off_y = slab_cells(index)
        upper = index // halves
        window = jnp.floor(col * (1.0 / INNER))
        local = col - window * INNER
        near = overlap(row_iota(FINE, both) - local, off_x, wide).astype(bf16)
        gap = jnp.zeros((LANES - FINE, both), bf16)
        hot = jnp.where(row_iota(coarse_rows, both) == window, 1.0, 0.0).astype(bf16)
        fine_part = dot(xf[...], jnp.concatenate([near, gap, near, gap], 0))
        coarse_part = dot(xg[...], jnp.concatenate([hot, hot], 0))
        along = fine_part[:LANES] * coarse_part[:LANES] - fine_part[LANES:] * coarse_part[LANES:]
        waves = jnp.concatenate(split(along), 0)
        start = (index * slab_rows).astype(f32)
        flip = upper.astype(f32)
        ladder = row_iota(slab_rows, both)
        place = start + ladder + flip * (slab_rows - 1.0 - 2.0 * ladder)
        tall = overlap(place - row, off_y, high).astype(bf16)
        flip_next = ((index + 1) // halves).astype(f32)
        steps = row_iota(8, both)
        place = start + slab_rows + steps + flip_next * (7.0 - 2.0 * steps)
        above = overlap(place - row, off_y, high)
        masks = [jnp.where(region == g, 1.0, 0.0) for g in range(regions)]
        above = jnp.concatenate([above * mask for mask in masks], 0).astype(bf16)
        stack = jnp.concatenate([tall * mask.astype(bf16) for mask in masks] + [above], 0)
        result = dot(stack, waves, ((1,), (1,)))
        result = result[:, :LANES] + result[:, LANES:]
        tile = index + upper * (2 * halves - 1 - 2 * index)
        base = pl.multiple_of(tile * slab_rows, slab_rows)
        for g in range(regions):
            lanes = pl.ds(g * LANES, LANES)
            draw[upper, pl.ds(base, slab_rows), lanes] = result[g * slab_rows : (g + 1) * slab_rows]
        carry[index] = result[regions * slab_rows :]
        return 0

    lax.fori_loop(0, slab_count, spread, 0)

    def hand_up(index, _):
        upper = index // halves
        tile = index + upper * (2 * halves - 1 - 2 * index)
        edge = pl.multiple_of(tile * slab_rows + upper * (slab_rows - 8), 8)
        for g in range(regions):
            lanes = pl.ds(g * LANES, LANES)
            draw[upper, pl.ds(edge, 8), lanes] += carry[index - 1, g * 8 : (g + 1) * 8, :]
        return 0

    lax.fori_loop(1, slab_count, hand_up, 0)

    def fold(step, _):
        at = pl.ds(pl.multiple_of(step * 64, 64), 64)
        lower, upper = draw[0, at, :], draw[1, at, :]
        foh[0, at, :], fol[0, at, :] = split(lower + upper)
        foh[1, at, :], fol[1, at, :] = split(lower - upper)
        return 0

    lax.fori_loop(0, half // 64, fold, 0)

    step_size = math.pi / length
    energy_acc[...] = jnp.zeros_like(energy_acc)
    chunk = 256
    kx = 2 * ((spot % halves) * LANES + lax.broadcasted_iota(jnp.int32, (chunk, LANES), 1)) + spot // halves
    kx = kx.astype(f32)

    def transform(step, _):
        parity = step // (half // chunk)
        first = (step % (half // chunk)) * chunk
        at = pl.ds(pl.multiple_of(first, chunk), chunk)
        high, low = xch[parity, at, :], xcl[parity, at, :]
        spectrum = dot(high, foh[parity]) + (dot(high, fol[parity]) + dot(low, foh[parity]))
        ky = (2 * (first + lax.broadcasted_iota(jnp.int32, (chunk, LANES), 0)) + parity).astype(f32)
        squared = kx * kx + ky * ky
        at_anchor = squared == 0.0
        scale = jnp.where(kx == 0.0, 1.0 / length, 2.0 / length) * jnp.where(ky == 0.0, 1.0 / length, 2.0 / length)
        weight = jnp.where(
            at_anchor, 0.0, scale / (step_size * step_size * jnp.where(at_anchor, 1.0, squared))
        )
        weight_x = weight * (step_size * kx)
        weight_y = weight * (step_size * ky)
        energy = energy_acc[...]
        for g in range(regions):
            lanes = pl.ds(g * LANES, LANES)
            part = spectrum[:, g * LANES : (g + 1) * LANES]
            hxh[parity, at, lanes], hxl[parity, at, lanes] = split(part * weight_x)
            hyh[parity, at, lanes], hyl[parity, at, lanes] = split(part * weight_y)
            energy += fold_rows(part * part * weight)
        energy_acc[...] = energy
        return 0

    lax.fori_loop(0, 2 * (half // chunk), transform, 0)

    def data_copy(index, target, source, place):
        return pltpu.make_async_remote_copy(
            src_ref=send_buf.at[index, target], dst_ref=recv_buf.at[index, source],
            send_sem=data_send.at[index, target], recv_sem=data_recv.at[index, source],
            device_id=to(side * group + place), device_id_type=pl.DeviceIdType.MESH,
        )

    def scale_copy(index, target, source, place):
        return pltpu.make_async_remote_copy(
            src_ref=send_scale.at[index, target], dst_ref=recv_scale.at[index, source],
            send_sem=scale_send.at[index, target], recv_sem=scale_recv.at[index, source],
            device_id=to(side * group + place), device_id_type=pl.DeviceIdType.MESH,
        )

    tiles = group // 4

    def inverse(step, _, index, th, tl, vh, vl):
        tile = (spot // 4 + step + 1) % tiles
        at = pl.ds(pl.multiple_of(tile * (4 * rows), 4 * rows), 4 * rows)
        value = None
        for parity in range(2):
            high, low = th[parity, at, :], tl[parity, at, :]
            term = dot(high, vh[parity]) + (dot(high, vl[parity]) + dot(low, vh[parity]))
            value = term if value is None else value + term
        for part in range(4):
            block = value[part * rows : (part + 1) * rows]
            top = jnp.maximum(jnp.max(jnp.abs(block), axis=0, keepdims=True), 1e-30)
            code = jnp.round(block * (CODE_TOP / top)).astype(jnp.int32).astype(jnp.int16)
            send_buf[index, tile * 4 + part] = code
            send_scale[index, tile * 4 + part] = jnp.broadcast_to(top * (1.0 / CODE_TOP), (2, regions * LANES))
        for part in range(4):
            target = tile * 4 + part

            @pl.when(target != spot)
            def _():
                data_copy(index, target, spot, target).start()
                scale_copy(index, target, spot, target).start()

            @pl.when(target == spot)
            def _():
                recv_buf[index, spot] = send_buf[index, spot]
                recv_scale[index, spot] = send_scale[index, spot]

        return 0

    for index, (th, tl, vh, vl) in enumerate(((ych, ycl, hxh, hxl), (ysh, ysl, hyh, hyl))):
        lax.fori_loop(
            0, tiles, functools.partial(inverse, index=index, th=th, tl=tl, vh=vh, vl=vl), 0
        )

    own = slab_cells(slab)
    under = slab_cells((slab + slab_count - 1) % slab_count)
    start = (slab * slab_rows + core * rows).astype(f32)
    for count, ref, (row, _, _, high, region, _, off_y) in ((rows, yown, own), (8, ybelow, under)):
        reach = overlap(start + row_iota(count, both) - row, off_y, high)
        for g in range(regions):
            ref[pl.ds(g * count, count), :] = jnp.where(region == g, reach, 0.0).astype(bf16)

    def columns(step, _):
        at = pl.ds(pl.multiple_of(step * 64, 64), 64)
        for part in range(2):
            spots = row_iota(64, both) + (step * 64 + part * half).astype(f32)
            for ref, (_, col, wide, _, _, off_x, _) in ((ych, own), (ycl, under)):
                ref[part, at, :] = overlap(spots - col, off_x, wide).astype(bf16)
        return 0

    lax.fori_loop(0, half // 64, columns, 0)
    excess_acc[...] = jnp.zeros_like(excess_acc)
    area_acc[...] = jnp.zeros_like(area_acc)

    def measure(step, _):
        part = step // (half // 256)
        at = pl.ds(pl.multiple_of((step % (half // 256)) * 256, 256), 256)
        density = dot(yown[...], ych[part, at, :], ((1,), (1,)))
        extra = dot(ybelow[...], ycl[part, at, :], ((1,), (1,)))
        excess, area = excess_acc[...], area_acc[...]
        for g in range(regions):
            block = density[g * rows : (g + 1) * rows]
            for piece in (block[:8] + extra[g * 8 : (g + 1) * 8], block[8:]):
                area += fold_rows(piece)
                excess += fold_rows(jnp.maximum(piece - 1.0, 0.0))
        excess_acc[...], area_acc[...] = excess, area
        return 0

    lax.fori_loop(0, length // 256, measure, 0)

    lane = lax.broadcasted_iota(jnp.int32, (8, LANES), 1)
    sums = jnp.where(lane == 0, jnp.sum(excess_acc[...]), 0.0)
    sums = jnp.where(lane == 1, jnp.sum(area_acc[...]), sums)
    sums = jnp.where(lane == 2, jnp.sum(energy_acc[...]) * (0.5 / (length * length)), sums)
    scal_out[...] = sums
    scal_in[me] = sums

    def scal_copy(step, source):
        return pltpu.make_async_remote_copy(
            src_ref=scal_out, dst_ref=scal_in.at[source], send_sem=scal_send.at[step],
            recv_sem=scal_recv.at[source], device_id=to((me + step) % device_count),
            device_id_type=pl.DeviceIdType.MESH,
        )

    def send_sums(step, _):
        scal_copy(step, me).start()
        return 0

    lax.fori_loop(1, device_count, send_sums, 0)
    lax.fori_loop(0, half // INNER, lambda s, c: build_x(s, ysh, ysl, 1), 0)

    def unpack(step, _, index):
        source = (spot + step) % group

        @pl.when(source != spot)
        def _():
            data_copy(index, source, source, source).wait_recv()
            scale_copy(index, source, source, source).wait_recv()

        across = source // 4
        lanes = pl.ds(pl.multiple_of((source % 4) * LANES, LANES), LANES)
        value = recv_buf[index, source].astype(jnp.int32).astype(f32) * recv_scale[index, source, :1, :]
        for g in range(regions):
            at = pl.ds(pl.multiple_of(across * (regions * rows) + g * rows, rows), rows)
            foh[index, at, lanes], fol[index, at, lanes] = split(value[:, g * LANES : (g + 1) * LANES])
        return 0

    high_rows = regions * rows
    mirror = LANES - 1 - lax.broadcasted_iota(jnp.int32, (high_rows, LANES), 1)
    wide = 256

    def finish(step, _, index, th, tl, out):
        at = pl.ds(pl.multiple_of(step * wide, wide), wide)
        sums = []
        for parity in range(2):
            total = None
            for block in range(2):
                pick = pl.ds((parity * 2 + block) * high_rows, high_rows)
                high, low = foh[index, pick, :], fol[index, pick, :]
                depth = pl.ds(block * 512, 512)
                left, right = th[parity, depth, at], tl[parity, depth, at]
                term = dot(high, left) + (dot(high, right) + dot(low, left))
                total = term if total is None else total + term
            sums.append(total)
        even, odd = sums
        straight = even + odd
        back = even - odd if index else odd - even
        rounded[:, at] = straight.astype(bf16)
        for g in range(regions):
            out[g, :, at] = straight[g * rows : (g + 1) * rows]
        for part in range(wide // LANES):
            tile = jnp.take_along_axis(
                back[:, part * LANES : (part + 1) * LANES], mirror, axis=1, mode="promise_in_bounds"
            )
            far = pl.ds(pl.multiple_of(length - (part + 1) * LANES - step * wide, LANES), LANES)
            rounded[:, far] = tile.astype(bf16)
            for g in range(regions):
                out[g, :, far] = tile[g * rows : (g + 1) * rows]
        return 0

    leaving = []
    for index, (th, tl, out, leave) in enumerate(((ysh, ysl, field_x, out_x), (xch, xcl, field_y, out_y))):
        lax.fori_loop(0, group, functools.partial(unpack, index=index), 0)
        lax.fori_loop(0, half // wide, functools.partial(finish, index=index, th=th, tl=tl, out=out), 0)
        leaving.append(pltpu.make_async_copy(out, leave, out_sem.at[index]))
        leaving[-1].start()
        low_rows = jnp.concatenate([out[g, :8, :] for g in range(regions)], 0).astype(bf16)
        total = dot(rounded[:, :half], ych[0]) + dot(rounded[:, half:], ych[1])
        extra = dot(low_rows[:, :half], ycl[0]) + dot(low_rows[:, half:], ycl[1])
        total = jnp.sum(total * yown[...].astype(f32), axis=0, keepdims=True)
        extra = jnp.sum(extra * ybelow[...].astype(f32), axis=0, keepdims=True)
        for part in range(2):
            part_own[part, pl.ds(index, 1), :] = total[:, part * cells : (part + 1) * cells]
            part_below[part, pl.ds(index, 1), :] = extra[:, part * cells : (part + 1) * cells]

    def sibling_copy():
        return pltpu.make_async_remote_copy(
            src_ref=part_own.at[1 - core], dst_ref=part_sib, send_sem=part_send.at[0],
            recv_sem=part_recv.at[0], device_id=(slab, 1 - core), device_id_type=pl.DeviceIdType.MESH,
        )

    def down_copy(part):
        return pltpu.make_async_remote_copy(
            src_ref=part_below.at[part], dst_ref=part_up, send_sem=part_send.at[1 + part],
            recv_sem=part_recv.at[1], device_id=(lax.max(slab - 1, 0), part),
            device_id_type=pl.DeviceIdType.MESH,
        )

    sibling_copy().start()

    @pl.when((core == 0) & (slab > 0))
    def _():
        down_copy(0).start()
        down_copy(1).start()

    def take_sums(step, _):
        scal_copy(step, (me + step) % device_count).wait_recv()
        return 0

    lax.fori_loop(1, device_count, take_sums, 0)
    total = scal_in[0]
    for source in range(1, device_count):
        total += scal_in[source]
    scalars[...] = jnp.where(lane == 3, total[:, :1] / total[:, 1:2], total)
    sibling_copy().wait_recv()
    force[...] = (part_own[core] + part_sib[...])[:2]

    @pl.when(slab < slab_count - 1)
    def _():
        down_copy(0).wait_recv()
        force[...] += part_up[:2, :]

    def drain(step, _):
        cell_copy(step).wait_send()
        scal_copy(step, me).wait_send()
        return 0

    lax.fori_loop(1, device_count, drain, 0)

    def drain_data(step, _):
        target = (spot + step) % group
        for index in range(2):
            data_copy(index, target, spot, target).wait_send()
            scale_copy(index, target, spot, target).wait_send()
        return 0

    lax.fori_loop(1, group, drain_data, 0)
    sibling_copy().wait_send()

    @pl.when((core == 0) & (slab > 0))
    def _():
        down_copy(0).wait_send()
        down_copy(1).wait_send()

    for copy in leaving:
        copy.wait()


def hand_out(in_x, in_y, in_force, in_scalars, out_x, out_y, force, energy, overflow):
    out_x[...] = in_x[...]
    out_y[...] = in_y[...]
    force[...] = in_force[...]
    energy[0, 0] = in_scalars[0, 2]
    overflow[0, 0] = in_scalars[0, 3]


def fused_body(cell_row, cell_col, cell_width, cell_height, cell_region, cell_offset):
    slab_count = lax.axis_size("slab")
    length, regions = M, REGIONS
    cells = cell_row.shape[0]
    half, group = length // 2, slab_count
    device_count = 2 * slab_count
    rows = length // device_count
    f32, bf16 = jnp.float32, jnp.bfloat16
    consts = [jnp.asarray(t) for t in small_tables(length)]
    vmem = pltpu.VMEM
    basis = vmem((2, half, half), bf16)
    panel = vmem((2, half, regions * LANES), bf16)
    sems = pltpu.SemaphoreType.DMA
    scratch = (
        [vmem((8, cells), f32)]
        + [vmem((regions, rows, length), f32)] * 2
        + [vmem((device_count, 8, cells), f32)]
        + [basis] * 6
        + [vmem((2, half, regions * LANES), f32)]
        + [panel] * 6
        + [
            vmem((2, group, rows, regions * LANES), jnp.int16),
            vmem((2, group, 2, regions * LANES), f32),
            vmem((2, group, rows, regions * LANES), jnp.int16),
            vmem((2, group, 2, regions * LANES), f32),
            vmem((regions * rows, length), bf16),
            vmem((2 * LANES, 2 * LANES), bf16),
            vmem((2 * LANES, 2 * (length // INNER)), bf16),
            vmem((slab_count, 8 * regions, LANES), f32),
            vmem((regions * rows, 2 * cells), bf16),
            vmem((8 * regions, 2 * cells), bf16),
            vmem((8, LANES), f32),
            vmem((8, 256), f32),
            vmem((8, 256), f32),
            vmem((8, LANES), f32),
            vmem((device_count, 8, LANES), f32),
            vmem((2, 8, cells), f32),
            vmem((2, 8, cells), f32),
            vmem((8, cells), f32),
            vmem((8, cells), f32),
            sems((device_count,)),
            sems((device_count,)),
            sems((2, group)),
            sems((2, group)),
            sems((2, group)),
            sems((2, group)),
            sems((device_count,)),
            sems((device_count,)),
            sems((3,)),
            sems((2,)),
            sems((2,)),
        ]
    )
    whole = pl.BlockSpec(memory_space=vmem)
    anywhere = pl.BlockSpec(memory_space=pl.ANY)
    field = jax.ShapeDtypeStruct((regions, rows, length), f32)
    field_x, field_y, force, scalars = pl.pallas_call(
        functools.partial(fused_kernel, slab_count, length, cells, regions),
        out_shape=(
            field,
            field,
            jax.ShapeDtypeStruct((2, cells), f32),
            jax.ShapeDtypeStruct((8, LANES), f32),
        ),
        in_specs=[whole] * (6 + len(consts)),
        out_specs=(anywhere, anywhere, whole, whole),
        scratch_shapes=scratch,
        compiler_params=pltpu.CompilerParams(
            collective_id=0, has_side_effects=True, vmem_limit_bytes=67043328
        ),
    )(cell_row, cell_col, cell_width, cell_height, cell_region, cell_offset, *consts)
    block = pl.BlockSpec((1, rows, length), lambda g: (g, 0, 0))
    small = pl.BlockSpec((2, cells), lambda g: (0, 0))
    number = pl.BlockSpec((1, 1), lambda g: (0, 0), memory_space=pltpu.SMEM)
    single = jax.ShapeDtypeStruct((1, 1), f32)
    field_x, field_y, force, energy, overflow = pl.pallas_call(
        hand_out,
        grid=(regions,),
        out_shape=(field, field, jax.ShapeDtypeStruct((2, cells), f32), single, single),
        in_specs=[block, block, small, pl.BlockSpec((8, LANES), lambda g: (0, 0), memory_space=pltpu.SMEM)],
        out_specs=(block, block, small, number, number),
    )(field_x, field_y, force, scalars)
    return field_x, field_y, force, energy.reshape(()), overflow.reshape(())


def fits(mesh):
    slab_count = mesh.shape["slab"]
    return mesh.shape["cell"] == 2 and slab_count % 8 == 0 and M == slab_count * LANES


def solution(mesh):
    return jax.shard_map(
        fused_body if fits(mesh) else body,
        mesh=mesh,
        in_specs=(
            P(("slab", "cell")),
            P(("slab", "cell")),
            P(("slab", "cell")),
            P(("slab", "cell")),
            P(("slab", "cell")),
            P(None, ("slab", "cell")),
        ),
        out_specs=(
            P(None, ("slab", "cell"), None),
            P(None, ("slab", "cell"), None),
            P(None, ("slab", "cell")),
            P(),
            P(),
        ),
        check_vma=False,
    )
```

```python
import functools
import math

import jax
import jax.numpy as jnp
import numpy as np
from jax import lax
from jax.experimental import pallas as pl
from jax.experimental.pallas import tpu as pltpu
from jax.sharding import PartitionSpec as P

M = 2048
REGIONS = 4
SEND_SCALE = 0.125


def shifted(value, axis, steps):
    count = lax.axis_size(axis)
    first, last = (max(0, -steps), min(count, count - steps))
    return lax.ppermute(value, axis, [(source, source + steps) for source in range(first, last)])


def intersect(offset_bins, fraction, extent):
    high_edge = jnp.minimum(offset_bins + 1.0, fraction + extent)
    low_edge = jnp.maximum(offset_bins, fraction)
    return jnp.maximum(high_edge - low_edge, 0.0).astype(jnp.bfloat16)


def basis_tables(length):
    inner = 32
    outer = length // 2 // inner
    position = 2 * lax.iota(jnp.int32, length) + 1

    def small(freq):
        phase = freq[..., None] * position % (4 * length)
        angle = phase.astype(jnp.float32) * (math.pi / (2.0 * length))
        return jnp.cos(angle), jnp.sin(angle)

    coarse_cos, coarse_sin = small(2 * inner * lax.iota(jnp.int32, outer))
    parity = lax.iota(jnp.int32, 2)[:, None]
    fine_cos, fine_sin = small(2 * lax.iota(jnp.int32, inner)[None, :] + parity)
    coarse_cos, coarse_sin, fine_cos, fine_sin = lax.optimization_barrier(
        (coarse_cos, coarse_sin, fine_cos, fine_sin)
    )
    def build(left_a, right_a, left_b, right_b, sign):
        step_rows = min(4, outer) * inner

        def kernel(la, ra, lb, rb, out):
            step = pl.program_id(1)
            for part in range(step_rows // inner):
                at = pl.ds(step * (step_rows // inner) + part, 1)
                value = la[at, :] * ra[0] + sign * (lb[at, :] * rb[0])
                value = value * math.sqrt(2.0 / length)
                if part == 0:
                    first = (pl.program_id(0) == 0) & (step == 0)
                    here = lax.broadcasted_iota(jnp.int32, (inner, length), 0) == 0
                    value = jnp.where(first & here, value * math.sqrt(0.5), value)
                out[pl.ds(part * inner, inner), :] = value

        small_spec = pl.BlockSpec((outer, length), lambda p, i: (0, 0))
        fine_spec = pl.BlockSpec((1, inner, length), lambda p, i: (p, 0, 0))
        steps = outer * inner // step_rows
        return pl.pallas_call(
            kernel,
            out_shape=jax.ShapeDtypeStruct((length, length), jnp.float32),
            grid=(2, steps),
            in_specs=[small_spec, fine_spec, small_spec, fine_spec],
            out_specs=pl.BlockSpec((step_rows, length), lambda p, i: (p * steps + i, 0)),
            cost_estimate=pl.CostEstimate(
                flops=4 * length * length, bytes_accessed=4 * length * length, transcendentals=0
            ),
        )(left_a, right_a, left_b, right_b)

    cosine = build(coarse_cos, fine_cos, coarse_sin, fine_sin, -1.0)
    sine = build(coarse_sin, fine_cos, coarse_cos, fine_sin, 1.0)
    return cosine, sine


def frequency_order(index, length):
    half = length // 2
    return jnp.where(index < half, 2 * index, 2 * (index - half) + 1)


def matmul(left, right, contract):
    return lax.dot_general(
        left,
        right,
        (contract, ((), ())),
        precision=lax.Precision.HIGH,
        preferred_element_type=jnp.float32,
    )


def body(cell_row, cell_col, cell_width, cell_height, cell_region, cell_offset):
    slab_count = lax.axis_size("slab")
    cell_count = lax.axis_size("cell")
    slab_index = lax.axis_index("slab")
    cell_index = lax.axis_index("cell")
    device_count = slab_count * cell_count
    length = M
    regions = REGIONS
    own_regions = regions // cell_count
    rows = length // device_count
    width = length // slab_count
    cells = cell_row.shape[0]
    base_row = (slab_index * cell_count + cell_index) * rows
    everyone = ("slab", "cell")
    cosine, sine = basis_tables(length)

    table = jnp.concatenate(
        [jnp.stack([cell_row, cell_col, cell_width, cell_height, cell_region]).astype(jnp.float32), cell_offset]
    )
    slab_cells = lax.all_gather(table, "cell", axis=1, tiled=True)
    below = shifted(slab_cells, "slab", 1)
    seen = jnp.concatenate([slab_cells, below], axis=1)
    row, col, wide, high, region, off_x, off_y = [seen[i][:, None] for i in range(7)]
    natural = lax.iota(jnp.float32, length)[None, :]
    x_intersect = intersect(natural - col, off_x, wide)
    y_bins = base_row.astype(jnp.float32) + lax.iota(jnp.float32, rows)[None, :] - row
    y_intersect = intersect(y_bins, off_y, high)
    region_hot = region == lax.iota(jnp.float32, regions)[None, :]
    y_region = jnp.where(region_hot[:, :, None], y_intersect[:, None, :], jnp.bfloat16(0)).reshape(
        seen.shape[1], regions * rows
    )
    density = lax.dot_general(
        y_region, x_intersect, (((0,), (0,)), ((), ())), preferred_element_type=jnp.float32
    )
    excess_local = jnp.sum(jnp.maximum(density - 1.0, 0.0))
    area_local = jnp.sum(density)

    by_freq_x = matmul(density, cosine, ((1,), (1,)))
    outgoing = by_freq_x.reshape(cell_count, own_regions, rows, slab_count, width)
    outgoing = outgoing.astype(jnp.float16)
    outgoing = outgoing.transpose(3, 0, 2, 1, 4).reshape(device_count, rows, own_regions * width)
    crossed = lax.all_to_all(outgoing, everyone, split_axis=0, concat_axis=0, tiled=True)
    crossed, sine = lax.optimization_barrier((crossed, sine))
    crossed = crossed.reshape(length, own_regions * width).astype(jnp.float32)
    spectrum = matmul(crossed, cosine, ((0,), (1,)))

    ky_int = frequency_order(lax.iota(jnp.int32, length), length)[None, :]
    kx_int = frequency_order(slab_index * width + lax.iota(jnp.int32, width), length)
    kx_int = jnp.tile(kx_int, own_regions)[:, None]
    kx, ky = kx_int.astype(jnp.float32), ky_int.astype(jnp.float32)
    at_anchor = kx_int + ky_int == 0
    step_size = math.pi / length
    squared = kx * kx + ky * ky
    potential_hat = jnp.where(
        at_anchor, 0.0, spectrum / (step_size * step_size * jnp.where(at_anchor, 1.0, squared))
    )
    energy_local = jnp.sum(spectrum * potential_hat) / (length * length)
    along_x = matmul(potential_hat * (step_size * kx * SEND_SCALE), cosine, ((1,), (0,)))
    along_y = matmul(potential_hat * (step_size * ky * SEND_SCALE), sine, ((1,), (0,)))

    def back(along):
        blocks = along.astype(jnp.float16).T.reshape(device_count, rows, own_regions * width)
        home = lax.all_to_all(blocks, everyone, split_axis=0, concat_axis=0, tiled=True)
        home = home.reshape(slab_count, cell_count, rows, own_regions, width)
        home = home.transpose(1, 3, 2, 0, 4).reshape(regions * rows, length)
        return home.astype(jnp.float32) * (1.0 / SEND_SCALE)

    home_x = back(along_x)
    home_y = back(along_y)
    sums = jnp.stack([excess_local, area_local, energy_local])
    sums, home_y = lax.optimization_barrier((sums, home_y))
    sums = jnp.broadcast_to(sums, (device_count, 3))
    sums = lax.all_to_all(sums, everyone, split_axis=0, concat_axis=0, tiled=True)
    field_x = matmul(home_x, sine, ((1,), (0,)))
    field_y = matmul(home_y, cosine, ((1,), (0,)))

    def pushed(field):
        sampled = lax.dot_general(
            x_intersect,
            field.astype(jnp.bfloat16),
            (((1,), (1,)), ((), ())),
            preferred_element_type=jnp.float32,
        )
        return jnp.sum(sampled * y_region.astype(jnp.float32), axis=1)

    partial = jnp.stack([pushed(field_x), pushed(field_y)])
    here, beneath = partial[:, : cells * cell_count], partial[:, cells * cell_count :]
    here = here + shifted(beneath, "slab", -1)
    here = here.reshape(2, cell_count, cells).transpose(1, 0, 2)
    cell_force = jnp.sum(lax.all_to_all(here, "cell", split_axis=0, concat_axis=0), axis=0)
    excess, area, energy = jnp.sum(sums, axis=0)
    shape = (regions, rows, length)
    return (field_x.reshape(shape), field_y.reshape(shape), cell_force, energy, excess / area)


INNER = 32
FINE = 48
LANES = 128
CODE_TOP = 32000.0


def trig(phase, length):
    angle = (phase % (4 * length)) * (math.pi / (2.0 * length))
    return np.cos(angle).astype(np.float32), np.sin(angle).astype(np.float32)


def small_tables(length):
    half = length // 2
    order = np.concatenate([2 * np.arange(half), 2 * np.arange(half) + 1])[None, :]
    coarse = np.arange(length // INNER)[:, None] * (2 * INNER)
    fine = 2 * np.arange(FINE)[:, None] + 1
    position = 2 * np.arange(half)[None, :] + 1
    freq_coarse = np.arange(half // INNER)[:, None] * (2 * INNER)
    freq_fine = (np.arange(2)[:, None, None] + 2 * np.arange(INNER)[None, :, None]) * position[None]
    return (
        trig(coarse * order, length)
        + trig(fine * order, length)
        + trig(freq_coarse * position, length)
        + trig(freq_fine, length)
    )


def split(value):
    high = value.astype(jnp.bfloat16)
    return high, (value - high.astype(jnp.float32)).astype(jnp.bfloat16)


def dot(left, right, contract=((1,), (0,))):
    return lax.dot_general(left, right, (contract, ((), ())), preferred_element_type=jnp.float32)


def overlap(steps, fraction, extent):
    high_edge = jnp.minimum(steps + 1.0, fraction + extent)
    return jnp.maximum(high_edge - jnp.maximum(steps, fraction), 0.0)


def row_iota(rows, columns):
    return lax.broadcasted_iota(jnp.int32, (rows, columns), 0).astype(jnp.float32)


def fold_rows(value):
    return jnp.sum(value.reshape(value.shape[0] // 8, 8, value.shape[1]), axis=0)


def fused_kernel(
    slab_count, length, cells, regions,
    cell_row, cell_col, cell_width, cell_height, cell_region, cell_offset,
    src_0, src_1, src_2, src_3, src_4, src_5, src_6, src_7,
    out_x, out_y, force, scalars,
    ccos, csin, fcos, fsin, gcos, gsin, hcos, hsin, table, field_x, field_y, cells_all, xch, xcl, ych, ycl, ysh, ysl, draw, foh, fol, hxh, hxl, hyh, hyl,
    send_buf, send_scale, recv_buf, recv_scale, rounded, xf, xg, carry, yown, ybelow,
    energy_acc, excess_acc, area_acc, scal_out, scal_in, part_own, part_below, part_sib, part_up,
    cell_send, cell_recv, data_send, data_recv, scale_send, scale_recv,
    scal_send, scal_recv, part_send, part_recv, out_sem, trig_sem,
):
    half = length // 2
    halves = slab_count // 2
    group = slab_count
    slab_rows = length // slab_count
    rows = slab_rows // 2
    both = 2 * cells
    device_count = 2 * slab_count
    slab = lax.axis_index("slab")
    core = lax.axis_index("cell")
    me = slab * 2 + core
    side = slab // halves
    spot = (slab % halves) * 2 + core
    f32, bf16 = jnp.float32, jnp.bfloat16

    def to(index):
        return (index // 2, index % 2)

    def neighbour(step):
        return ((slab + step // 2) % slab_count, (core + step) % 2)

    def cell_copy(step):
        return pltpu.make_async_remote_copy(
            src_ref=table, dst_ref=cells_all.at[me], send_sem=cell_send.at[step],
            recv_sem=cell_recv.at[me], device_id=neighbour(step),
            device_id_type=pl.DeviceIdType.MESH,
        )

    def cell_arrival(source):
        return pltpu.make_async_remote_copy(
            src_ref=table, dst_ref=cells_all.at[source], send_sem=cell_send.at[0],
            recv_sem=cell_recv.at[source], device_id=to((me + 1) % device_count),
            device_id_type=pl.DeviceIdType.MESH,
        )

    tables = [
        pltpu.make_async_copy(source, target, trig_sem.at[index])
        for index, (source, target) in enumerate(
            zip(
                (src_0, src_1, src_2, src_3, src_4, src_5, src_6, src_7),
                (ccos, csin, fcos, fsin, gcos, gsin, hcos, hsin),
            )
        )
    ]
    for copy in tables:
        copy.start()
    barrier = pltpu.get_barrier_semaphore()

    def greet(step, _):
        pl.semaphore_signal(
            barrier, inc=1, device_id=to((me + step) % device_count), device_id_type=pl.DeviceIdType.MESH
        )
        return 0

    lax.fori_loop(1, device_count, greet, 0)
    for index, ref in enumerate((cell_row, cell_col, cell_width, cell_height, cell_region)):
        table[pl.ds(index, 1), :] = ref[...].reshape(1, cells).astype(f32)
    table[5:7, :] = cell_offset[...]
    table[7:8, :] = jnp.zeros((1, cells), f32)
    pl.semaphore_wait(barrier, device_count - 1)

    def send_cells(step, _):
        cell_copy(step).start()
        return 0

    lax.fori_loop(1, device_count, send_cells, 0)
    cells_all[me] = table[...]
    for copy in tables:
        copy.wait()

    def rotate(cos_a, sin_a, cos_b, sin_b):
        return cos_a * cos_b - sin_a * sin_b, sin_a * cos_b + cos_a * sin_b

    def build_y(step, _):
        at = pl.ds(pl.multiple_of(step * INNER, INNER), INNER)
        row = pl.ds(side * (half // INNER) + step, 1)
        for parity in range(2):
            for part in range(half // 256):
                lanes = pl.ds(parity * half + part * 256, 256)
                out = pl.ds(part * 256, 256)
                cosine, sine = rotate(
                    ccos[row, lanes], csin[row, lanes], fcos[:INNER, lanes], fsin[:INNER, lanes]
                )
                ych[parity, at, out], ycl[parity, at, out] = split(cosine)
                ysh[parity, at, out], ysl[parity, at, out] = split(sine)
        return 0

    def build_x(step, high, low, pick):
        at = pl.ds(pl.multiple_of(step * INNER, INNER), INNER)
        row = pl.ds(step, 1)
        for parity in range(2):
            for part in range(half // 256):
                lanes = pl.ds(part * 256, 256)
                value = rotate(gcos[row, lanes], gsin[row, lanes], hcos[parity, :, lanes], hsin[parity, :, lanes])
                high[parity, at, lanes], low[parity, at, lanes] = split(value[pick])
        return 0

    lax.fori_loop(0, half // INNER, lambda s, c: build_x(s, xch, xcl, 0), 0)
    lax.fori_loop(0, half // INNER, build_y, 0)

    mine = pl.ds(pl.multiple_of(spot * LANES, LANES), LANES)
    coarse_rows = length // INNER
    for index, (fine_ref, coarse_ref) in enumerate(((fcos, ccos), (fsin, csin))):
        into = pl.ds(index * LANES, LANES)
        pad = jnp.zeros((LANES - FINE, LANES), f32)
        value = fine_ref[:, mine]
        high = value.astype(bf16).astype(f32)
        xf[into, :LANES] = jnp.concatenate([high, pad], 0).T.astype(bf16)
        xf[into, LANES:] = jnp.concatenate([value - high, pad], 0).T.astype(bf16)
        value = coarse_ref[:, mine]
        high = value.astype(bf16).astype(f32)
        xg[into, :] = jnp.concatenate([high, value - high], 0).T.astype(bf16)

    def slab_cells(index):
        block = jnp.concatenate([cells_all[2 * index], cells_all[2 * index + 1]], axis=1)
        return [block[i : i + 1, :] for i in range(7)]

    def spread(step, _):
        pair = [(slab + slab_count - 2 * step - back) % slab_count for back in range(2)]
        for index in pair:
            for part in range(2):

                @pl.when(2 * index + part != me)
                def _(source=2 * index + part):
                    cell_arrival(source).wait_recv()

        for index in pair:
            spread_slab(index)
        return 0

    def spread_slab(index):
        row, col, wide, high, region, off_x, off_y = slab_cells(index)
        upper = index // halves
        window = jnp.floor(col * (1.0 / INNER))
        local = col - window * INNER
        near = overlap(row_iota(FINE, both) - local, off_x, wide).astype(bf16)
        gap = jnp.zeros((LANES - FINE, both), bf16)
        hot = jnp.where(row_iota(coarse_rows, both) == window, 1.0, 0.0).astype(bf16)
        fine_part = dot(xf[...], jnp.concatenate([near, gap, near, gap], 0))
        coarse_part = dot(xg[...], jnp.concatenate([hot, hot], 0))
        along = fine_part[:LANES] * coarse_part[:LANES] - fine_part[LANES:] * coarse_part[LANES:]
        waves = jnp.concatenate(split(along), 0)
        start = (index * slab_rows).astype(f32)
        flip = upper.astype(f32)
        ladder = row_iota(slab_rows, both)
        place = start + ladder + flip * (slab_rows - 1.0 - 2.0 * ladder)
        tall = overlap(place - row, off_y, high).astype(bf16)
        flip_next = ((index + 1) // halves).astype(f32)
        steps = row_iota(8, both)
        place = start + slab_rows + steps + flip_next * (7.0 - 2.0 * steps)
        above = overlap(place - row, off_y, high)
        masks = [jnp.where(region == g, 1.0, 0.0) for g in range(regions)]
        above = jnp.concatenate([above * mask for mask in masks], 0).astype(bf16)
        stack = jnp.concatenate([tall * mask.astype(bf16) for mask in masks] + [above], 0)
        result = dot(stack, waves, ((1,), (1,)))
        result = result[:, :LANES] + result[:, LANES:]
        tile = index + upper * (2 * halves - 1 - 2 * index)
        base = pl.multiple_of(tile * slab_rows, slab_rows)
        for g in range(regions):
            lanes = pl.ds(g * LANES, LANES)
            draw[upper, pl.ds(base, slab_rows), lanes] = result[g * slab_rows : (g + 1) * slab_rows]
        carry[index] = result[regions * slab_rows :]

    lax.fori_loop(0, slab_count // 2, spread, 0)

    def hand_up(index, _):
        upper = index // halves
        tile = index + upper * (2 * halves - 1 - 2 * index)
        edge = pl.multiple_of(tile * slab_rows + upper * (slab_rows - 8), 8)
        for g in range(regions):
            lanes = pl.ds(g * LANES, LANES)
            draw[upper, pl.ds(edge, 8), lanes] += carry[index - 1, g * 8 : (g + 1) * 8, :]
        return 0

    lax.fori_loop(1, slab_count, hand_up, 0)

    def fold(step, _):
        at = pl.ds(pl.multiple_of(step * 64, 64), 64)
        lower, upper = draw[0, at, :], draw[1, at, :]
        foh[0, at, :], fol[0, at, :] = split(lower + upper)
        foh[1, at, :], fol[1, at, :] = split(lower - upper)
        return 0

    lax.fori_loop(0, half // 64, fold, 0)

    step_size = math.pi / length
    energy_acc[...] = jnp.zeros_like(energy_acc)
    chunk = 512
    kx = 2 * ((spot % halves) * LANES + lax.broadcasted_iota(jnp.int32, (chunk, LANES), 1)) + spot // halves
    kx = kx.astype(f32)

    def transform(step, _):
        parity = step // (half // chunk)
        first = (step % (half // chunk)) * chunk
        at = pl.ds(pl.multiple_of(first, chunk), chunk)
        high, low = xch[parity, at, :], xcl[parity, at, :]
        spectrum = dot(high, foh[parity]) + (dot(high, fol[parity]) + dot(low, foh[parity]))
        ky = (2 * (first + lax.broadcasted_iota(jnp.int32, (chunk, LANES), 0)) + parity).astype(f32)
        squared = kx * kx + ky * ky
        at_anchor = squared == 0.0
        scale = jnp.where(kx == 0.0, 1.0 / length, 2.0 / length) * jnp.where(ky == 0.0, 1.0 / length, 2.0 / length)
        weight = jnp.where(
            at_anchor, 0.0, scale / (step_size * step_size * jnp.where(at_anchor, 1.0, squared))
        )
        weight_x = weight * (step_size * kx)
        weight_y = weight * (step_size * ky)
        energy = energy_acc[...]
        for g in range(regions):
            lanes = pl.ds(g * LANES, LANES)
            part = spectrum[:, g * LANES : (g + 1) * LANES]
            hxh[parity, at, lanes], hxl[parity, at, lanes] = split(part * weight_x)
            hyh[parity, at, lanes], hyl[parity, at, lanes] = split(part * weight_y)
            energy += fold_rows(part * part * weight)
        energy_acc[...] = energy
        return 0

    lax.fori_loop(0, 2 * (half // chunk), transform, 0)

    def data_copy(index, target, source, place):
        return pltpu.make_async_remote_copy(
            src_ref=send_buf.at[index, target], dst_ref=recv_buf.at[index, source],
            send_sem=data_send.at[index, target], recv_sem=data_recv.at[index, source],
            device_id=to(side * group + place), device_id_type=pl.DeviceIdType.MESH,
        )

    def scale_copy(index, target, source, place):
        return pltpu.make_async_remote_copy(
            src_ref=send_scale.at[index, target], dst_ref=recv_scale.at[index, source],
            send_sem=scale_send.at[index, target], recv_sem=scale_recv.at[index, source],
            device_id=to(side * group + place), device_id_type=pl.DeviceIdType.MESH,
        )

    tiles = group // 4

    def inverse(step, _, index, th, tl, vh, vl):
        tile = (spot // 4 + step + 1) % tiles
        at = pl.ds(pl.multiple_of(tile * (4 * rows), 4 * rows), 4 * rows)
        value = None
        for parity in range(2):
            high, low = th[parity, at, :], tl[parity, at, :]
            term = dot(high, vh[parity]) + (dot(high, vl[parity]) + dot(low, vh[parity]))
            value = term if value is None else value + term
        for part in range(4):
            block = value[part * rows : (part + 1) * rows]
            top = jnp.maximum(jnp.max(jnp.abs(block), axis=0, keepdims=True), 1e-30)
            code = jnp.round(block * (CODE_TOP / top)).astype(jnp.int32).astype(jnp.int16)
            send_buf[index, tile * 4 + part] = code
            send_scale[index, tile * 4 + part] = jnp.broadcast_to(top * (1.0 / CODE_TOP), (2, regions * LANES))
        for part in range(4):
            target = tile * 4 + part

            @pl.when(target != spot)
            def _():
                data_copy(index, target, spot, target).start()
                scale_copy(index, target, spot, target).start()

            @pl.when(target == spot)
            def _():
                recv_buf[index, spot] = send_buf[index, spot]
                recv_scale[index, spot] = send_scale[index, spot]

        return 0

    for index, (th, tl, vh, vl) in enumerate(((ych, ycl, hxh, hxl), (ysh, ysl, hyh, hyl))):
        lax.fori_loop(
            0, tiles, functools.partial(inverse, index=index, th=th, tl=tl, vh=vh, vl=vl), 0
        )

    own = slab_cells(slab)
    under = slab_cells((slab + slab_count - 1) % slab_count)
    start = (slab * slab_rows + core * rows).astype(f32)
    for count, ref, (row, _, _, high, region, _, off_y) in ((rows, yown, own), (8, ybelow, under)):
        reach = overlap(start + row_iota(count, both) - row, off_y, high)
        for g in range(regions):
            ref[pl.ds(g * count, count), :] = jnp.where(region == g, reach, 0.0).astype(bf16)

    def columns(step, _):
        at = pl.ds(pl.multiple_of(step * 64, 64), 64)
        for part in range(2):
            spots = row_iota(64, both) + (step * 64 + part * half).astype(f32)
            for ref, (_, col, wide, _, _, off_x, _) in ((ych, own), (ycl, under)):
                ref[part, at, :] = overlap(spots - col, off_x, wide).astype(bf16)
        return 0

    lax.fori_loop(0, half // 64, columns, 0)
    excess_acc[...] = jnp.zeros_like(excess_acc)
    area_acc[...] = jnp.zeros_like(area_acc)

    def measure(step, _):
        part = step // (half // 256)
        at = pl.ds(pl.multiple_of((step % (half // 256)) * 256, 256), 256)
        density = dot(yown[...], ych[part, at, :], ((1,), (1,)))
        extra = dot(ybelow[...], ycl[part, at, :], ((1,), (1,)))
        excess, area = excess_acc[...], area_acc[...]
        for g in range(regions):
            block = density[g * rows : (g + 1) * rows]
            for piece in (block[:8] + extra[g * 8 : (g + 1) * 8], block[8:]):
                area += fold_rows(piece)
                excess += fold_rows(jnp.maximum(piece - 1.0, 0.0))
        excess_acc[...], area_acc[...] = excess, area
        return 0

    lax.fori_loop(0, length // 256, measure, 0)

    lane = lax.broadcasted_iota(jnp.int32, (8, LANES), 1)
    sums = jnp.where(lane == 0, jnp.sum(excess_acc[...]), 0.0)
    sums = jnp.where(lane == 1, jnp.sum(area_acc[...]), sums)
    sums = jnp.where(lane == 2, jnp.sum(energy_acc[...]) * (0.5 / (length * length)), sums)
    scal_out[...] = sums
    scal_in[me] = sums

    def scal_copy(step, source):
        return pltpu.make_async_remote_copy(
            src_ref=scal_out, dst_ref=scal_in.at[source], send_sem=scal_send.at[step],
            recv_sem=scal_recv.at[source], device_id=to((me + step) % device_count),
            device_id_type=pl.DeviceIdType.MESH,
        )

    def send_sums(step, _):
        scal_copy(step, me).start()
        return 0

    lax.fori_loop(1, device_count, send_sums, 0)
    lax.fori_loop(0, half // INNER, lambda s, c: build_x(s, ysh, ysl, 1), 0)

    def unpack(step, _, index):
        source = (spot + step) % group

        @pl.when(source != spot)
        def _():
            data_copy(index, source, source, source).wait_recv()
            scale_copy(index, source, source, source).wait_recv()

        across = source // 4
        lanes = pl.ds(pl.multiple_of((source % 4) * LANES, LANES), LANES)
        value = recv_buf[index, source].astype(jnp.int32).astype(f32) * recv_scale[index, source, :1, :]
        for g in range(regions):
            at = pl.ds(pl.multiple_of(across * (regions * rows) + g * rows, rows), rows)
            foh[index, at, lanes], fol[index, at, lanes] = split(value[:, g * LANES : (g + 1) * LANES])
        return 0

    high_rows = regions * rows
    mirror = LANES - 1 - lax.broadcasted_iota(jnp.int32, (high_rows, LANES), 1)
    wide = 256

    def finish(step, _, index, th, tl, out):
        at = pl.ds(pl.multiple_of(step * wide, wide), wide)
        sums = []
        for parity in range(2):
            total = None
            for block in range(2):
                pick = pl.ds((parity * 2 + block) * high_rows, high_rows)
                high, low = foh[index, pick, :], fol[index, pick, :]
                depth = pl.ds(block * 512, 512)
                left, right = th[parity, depth, at], tl[parity, depth, at]
                term = dot(high, left) + (dot(high, right) + dot(low, left))
                total = term if total is None else total + term
            sums.append(total)
        even, odd = sums
        straight = even + odd
        back = even - odd if index else odd - even
        rounded[:, at] = straight.astype(bf16)
        for g in range(regions):
            out[g, :, at] = straight[g * rows : (g + 1) * rows]
        for part in range(wide // LANES):
            tile = jnp.take_along_axis(
                back[:, part * LANES : (part + 1) * LANES], mirror, axis=1, mode="promise_in_bounds"
            )
            far = pl.ds(pl.multiple_of(length - (part + 1) * LANES - step * wide, LANES), LANES)
            rounded[:, far] = tile.astype(bf16)
            for g in range(regions):
                out[g, :, far] = tile[g * rows : (g + 1) * rows]
        return 0

    leaving = []
    for index, (th, tl, out, leave) in enumerate(((ysh, ysl, field_x, out_x), (xch, xcl, field_y, out_y))):
        lax.fori_loop(0, group, functools.partial(unpack, index=index), 0)
        lax.fori_loop(0, half // wide, functools.partial(finish, index=index, th=th, tl=tl, out=out), 0)
        leaving.append(pltpu.make_async_copy(out, leave, out_sem.at[index]))
        leaving[-1].start()
        low_rows = jnp.concatenate([out[g, :8, :] for g in range(regions)], 0).astype(bf16)
        total = dot(rounded[:, :half], ych[0]) + dot(rounded[:, half:], ych[1])
        extra = dot(low_rows[:, :half], ycl[0]) + dot(low_rows[:, half:], ycl[1])
        total = jnp.sum(total * yown[...].astype(f32), axis=0, keepdims=True)
        extra = jnp.sum(extra * ybelow[...].astype(f32), axis=0, keepdims=True)
        for part in range(2):
            part_own[part, pl.ds(index, 1), :] = total[:, part * cells : (part + 1) * cells]
            part_below[part, pl.ds(index, 1), :] = extra[:, part * cells : (part + 1) * cells]

    def sibling_copy():
        return pltpu.make_async_remote_copy(
            src_ref=part_own.at[1 - core], dst_ref=part_sib, send_sem=part_send.at[0],
            recv_sem=part_recv.at[0], device_id=(slab, 1 - core), device_id_type=pl.DeviceIdType.MESH,
        )

    def down_copy(part):
        return pltpu.make_async_remote_copy(
            src_ref=part_below.at[part], dst_ref=part_up, send_sem=part_send.at[1 + part],
            recv_sem=part_recv.at[1], device_id=(lax.max(slab - 1, 0), part),
            device_id_type=pl.DeviceIdType.MESH,
        )

    sibling_copy().start()

    @pl.when((core == 0) & (slab > 0))
    def _():
        down_copy(0).start()
        down_copy(1).start()

    def take_sums(step, _):
        scal_copy(step, (me + step) % device_count).wait_recv()
        return 0

    lax.fori_loop(1, device_count, take_sums, 0)
    total = scal_in[0]
    for source in range(1, device_count):
        total += scal_in[source]
    scalars[...] = jnp.where(lane == 3, total[:, :1] / total[:, 1:2], total)
    sibling_copy().wait_recv()
    force[...] = (part_own[core] + part_sib[...])[:2]

    @pl.when(slab < slab_count - 1)
    def _():
        down_copy(0).wait_recv()
        force[...] += part_up[:2, :]

    def drain(step, _):
        cell_copy(step).wait_send()
        scal_copy(step, me).wait_send()
        return 0

    lax.fori_loop(1, device_count, drain, 0)

    def drain_data(step, _):
        target = (spot + step) % group
        for index in range(2):
            data_copy(index, target, spot, target).wait_send()
            scale_copy(index, target, spot, target).wait_send()
        return 0

    lax.fori_loop(1, group, drain_data, 0)
    sibling_copy().wait_send()

    @pl.when((core == 0) & (slab > 0))
    def _():
        down_copy(0).wait_send()
        down_copy(1).wait_send()

    for copy in leaving:
        copy.wait()


def hand_out(in_x, in_y, in_force, in_scalars, out_x, out_y, force, energy, overflow):
    out_x[...] = in_x[...]
    out_y[...] = in_y[...]
    force[...] = in_force[...]
    energy[0, 0] = in_scalars[0, 2]
    overflow[0, 0] = in_scalars[0, 3]


def fused_body(cell_row, cell_col, cell_width, cell_height, cell_region, cell_offset):
    slab_count = lax.axis_size("slab")
    length, regions = M, REGIONS
    cells = cell_row.shape[0]
    half, group = length // 2, slab_count
    device_count = 2 * slab_count
    rows = length // device_count
    f32, bf16 = jnp.float32, jnp.bfloat16
    consts = [jnp.asarray(t) for t in small_tables(length)]
    vmem = pltpu.VMEM
    basis = vmem((2, half, half), bf16)
    panel = vmem((2, half, regions * LANES), bf16)
    sems = pltpu.SemaphoreType.DMA
    scratch = (
        [vmem(t.shape, f32) for t in consts]
        + [vmem((8, cells), f32)]
        + [vmem((regions, rows, length), f32)] * 2
        + [vmem((device_count, 8, cells), f32)]
        + [basis] * 6
        + [vmem((2, half, regions * LANES), f32)]
        + [panel] * 6
        + [
            vmem((2, group, rows, regions * LANES), jnp.int16),
            vmem((2, group, 2, regions * LANES), f32),
            vmem((2, group, rows, regions * LANES), jnp.int16),
            vmem((2, group, 2, regions * LANES), f32),
            vmem((regions * rows, length), bf16),
            vmem((2 * LANES, 2 * LANES), bf16),
            vmem((2 * LANES, 2 * (length // INNER)), bf16),
            vmem((slab_count, 8 * regions, LANES), f32),
            vmem((regions * rows, 2 * cells), bf16),
            vmem((8 * regions, 2 * cells), bf16),
            vmem((8, LANES), f32),
            vmem((8, 256), f32),
            vmem((8, 256), f32),
            vmem((8, LANES), f32),
            vmem((device_count, 8, LANES), f32),
            vmem((2, 8, cells), f32),
            vmem((2, 8, cells), f32),
            vmem((8, cells), f32),
            vmem((8, cells), f32),
            sems((device_count,)),
            sems((device_count,)),
            sems((2, group)),
            sems((2, group)),
            sems((2, group)),
            sems((2, group)),
            sems((device_count,)),
            sems((device_count,)),
            sems((3,)),
            sems((2,)),
            sems((2,)),
            sems((len(consts),)),
        ]
    )
    whole = pl.BlockSpec(memory_space=vmem)
    anywhere = pl.BlockSpec(memory_space=pl.ANY)
    field = jax.ShapeDtypeStruct((regions, rows, length), f32)
    field_x, field_y, force, scalars = pl.pallas_call(
        functools.partial(fused_kernel, slab_count, length, cells, regions),
        out_shape=(
            field,
            field,
            jax.ShapeDtypeStruct((2, cells), f32),
            jax.ShapeDtypeStruct((8, LANES), f32),
        ),
        in_specs=[whole] * 6 + [anywhere] * len(consts),
        out_specs=(anywhere, anywhere, whole, whole),
        scratch_shapes=scratch,
        compiler_params=pltpu.CompilerParams(
            collective_id=0, has_side_effects=True, vmem_limit_bytes=67043328
        ),
    )(cell_row, cell_col, cell_width, cell_height, cell_region, cell_offset, *consts)
    block = pl.BlockSpec((1, rows // 2, length), lambda g, r: (g, r, 0))
    small = pl.BlockSpec((2, cells), lambda g, r: (0, 0))
    number = pl.BlockSpec((1, 1), lambda g, r: (0, 0), memory_space=pltpu.SMEM)
    single = jax.ShapeDtypeStruct((1, 1), f32)
    field_x, field_y, force, energy, overflow = pl.pallas_call(
        hand_out,
        grid=(regions, 2),
        out_shape=(field, field, jax.ShapeDtypeStruct((2, cells), f32), single, single),
        in_specs=[block, block, small, pl.BlockSpec((8, LANES), lambda g, r: (0, 0), memory_space=pltpu.SMEM)],
        out_specs=(block, block, small, number, number),
    )(field_x, field_y, force, scalars)
    return field_x, field_y, force, energy.reshape(()), overflow.reshape(())


def fits(mesh):
    slab_count = mesh.shape["slab"]
    return mesh.shape["cell"] == 2 and slab_count % 8 == 0 and M == slab_count * LANES


def solution(mesh):
    return jax.shard_map(
        fused_body if fits(mesh) else body,
        mesh=mesh,
        in_specs=(
            P(("slab", "cell")),
            P(("slab", "cell")),
            P(("slab", "cell")),
            P(("slab", "cell")),
            P(("slab", "cell")),
            P(None, ("slab", "cell")),
        ),
        out_specs=(
            P(None, ("slab", "cell"), None),
            P(None, ("slab", "cell"), None),
            P(None, ("slab", "cell")),
            P(),
            P(),
        ),
        check_vma=False,
    )
```

```python
import functools
import math

import jax
import jax.numpy as jnp
import numpy as np
from jax import lax
from jax.experimental import pallas as pl
from jax.experimental.pallas import tpu as pltpu
from jax.sharding import PartitionSpec as P

M = 2048
REGIONS = 4
SEND_SCALE = 0.125


def shifted(value, axis, steps):
    count = lax.axis_size(axis)
    first, last = (max(0, -steps), min(count, count - steps))
    return lax.ppermute(value, axis, [(source, source + steps) for source in range(first, last)])


def intersect(offset_bins, fraction, extent):
    high_edge = jnp.minimum(offset_bins + 1.0, fraction + extent)
    low_edge = jnp.maximum(offset_bins, fraction)
    return jnp.maximum(high_edge - low_edge, 0.0).astype(jnp.bfloat16)


def basis_tables(length):
    inner = 32
    outer = length // 2 // inner
    position = 2 * lax.iota(jnp.int32, length) + 1

    def small(freq):
        phase = freq[..., None] * position % (4 * length)
        angle = phase.astype(jnp.float32) * (math.pi / (2.0 * length))
        return jnp.cos(angle), jnp.sin(angle)

    coarse_cos, coarse_sin = small(2 * inner * lax.iota(jnp.int32, outer))
    parity = lax.iota(jnp.int32, 2)[:, None]
    fine_cos, fine_sin = small(2 * lax.iota(jnp.int32, inner)[None, :] + parity)
    coarse_cos, coarse_sin, fine_cos, fine_sin = lax.optimization_barrier(
        (coarse_cos, coarse_sin, fine_cos, fine_sin)
    )
    def build(left_a, right_a, left_b, right_b, sign):
        step_rows = min(4, outer) * inner

        def kernel(la, ra, lb, rb, out):
            step = pl.program_id(1)
            for part in range(step_rows // inner):
                at = pl.ds(step * (step_rows // inner) + part, 1)
                value = la[at, :] * ra[0] + sign * (lb[at, :] * rb[0])
                value = value * math.sqrt(2.0 / length)
                if part == 0:
                    first = (pl.program_id(0) == 0) & (step == 0)
                    here = lax.broadcasted_iota(jnp.int32, (inner, length), 0) == 0
                    value = jnp.where(first & here, value * math.sqrt(0.5), value)
                out[pl.ds(part * inner, inner), :] = value

        small_spec = pl.BlockSpec((outer, length), lambda p, i: (0, 0))
        fine_spec = pl.BlockSpec((1, inner, length), lambda p, i: (p, 0, 0))
        steps = outer * inner // step_rows
        return pl.pallas_call(
            kernel,
            out_shape=jax.ShapeDtypeStruct((length, length), jnp.float32),
            grid=(2, steps),
            in_specs=[small_spec, fine_spec, small_spec, fine_spec],
            out_specs=pl.BlockSpec((step_rows, length), lambda p, i: (p * steps + i, 0)),
            cost_estimate=pl.CostEstimate(
                flops=4 * length * length, bytes_accessed=4 * length * length, transcendentals=0
            ),
        )(left_a, right_a, left_b, right_b)

    cosine = build(coarse_cos, fine_cos, coarse_sin, fine_sin, -1.0)
    sine = build(coarse_sin, fine_cos, coarse_cos, fine_sin, 1.0)
    return cosine, sine


def frequency_order(index, length):
    half = length // 2
    return jnp.where(index < half, 2 * index, 2 * (index - half) + 1)


def matmul(left, right, contract):
    return lax.dot_general(
        left,
        right,
        (contract, ((), ())),
        precision=lax.Precision.HIGH,
        preferred_element_type=jnp.float32,
    )


def body(cell_row, cell_col, cell_width, cell_height, cell_region, cell_offset):
    slab_count = lax.axis_size("slab")
    cell_count = lax.axis_size("cell")
    slab_index = lax.axis_index("slab")
    cell_index = lax.axis_index("cell")
    device_count = slab_count * cell_count
    length = M
    regions = REGIONS
    own_regions = regions // cell_count
    rows = length // device_count
    width = length // slab_count
    cells = cell_row.shape[0]
    base_row = (slab_index * cell_count + cell_index) * rows
    everyone = ("slab", "cell")
    cosine, sine = basis_tables(length)

    table = jnp.concatenate(
        [jnp.stack([cell_row, cell_col, cell_width, cell_height, cell_region]).astype(jnp.float32), cell_offset]
    )
    slab_cells = lax.all_gather(table, "cell", axis=1, tiled=True)
    below = shifted(slab_cells, "slab", 1)
    seen = jnp.concatenate([slab_cells, below], axis=1)
    row, col, wide, high, region, off_x, off_y = [seen[i][:, None] for i in range(7)]
    natural = lax.iota(jnp.float32, length)[None, :]
    x_intersect = intersect(natural - col, off_x, wide)
    y_bins = base_row.astype(jnp.float32) + lax.iota(jnp.float32, rows)[None, :] - row
    y_intersect = intersect(y_bins, off_y, high)
    region_hot = region == lax.iota(jnp.float32, regions)[None, :]
    y_region = jnp.where(region_hot[:, :, None], y_intersect[:, None, :], jnp.bfloat16(0)).reshape(
        seen.shape[1], regions * rows
    )
    density = lax.dot_general(
        y_region, x_intersect, (((0,), (0,)), ((), ())), preferred_element_type=jnp.float32
    )
    excess_local = jnp.sum(jnp.maximum(density - 1.0, 0.0))
    area_local = jnp.sum(density)

    by_freq_x = matmul(density, cosine, ((1,), (1,)))
    outgoing = by_freq_x.reshape(cell_count, own_regions, rows, slab_count, width)
    outgoing = outgoing.astype(jnp.float16)
    outgoing = outgoing.transpose(3, 0, 2, 1, 4).reshape(device_count, rows, own_regions * width)
    crossed = lax.all_to_all(outgoing, everyone, split_axis=0, concat_axis=0, tiled=True)
    crossed, sine = lax.optimization_barrier((crossed, sine))
    crossed = crossed.reshape(length, own_regions * width).astype(jnp.float32)
    spectrum = matmul(crossed, cosine, ((0,), (1,)))

    ky_int = frequency_order(lax.iota(jnp.int32, length), length)[None, :]
    kx_int = frequency_order(slab_index * width + lax.iota(jnp.int32, width), length)
    kx_int = jnp.tile(kx_int, own_regions)[:, None]
    kx, ky = kx_int.astype(jnp.float32), ky_int.astype(jnp.float32)
    at_anchor = kx_int + ky_int == 0
    step_size = math.pi / length
    squared = kx * kx + ky * ky
    potential_hat = jnp.where(
        at_anchor, 0.0, spectrum / (step_size * step_size * jnp.where(at_anchor, 1.0, squared))
    )
    energy_local = jnp.sum(spectrum * potential_hat) / (length * length)
    along_x = matmul(potential_hat * (step_size * kx * SEND_SCALE), cosine, ((1,), (0,)))
    along_y = matmul(potential_hat * (step_size * ky * SEND_SCALE), sine, ((1,), (0,)))

    def back(along):
        blocks = along.astype(jnp.float16).T.reshape(device_count, rows, own_regions * width)
        home = lax.all_to_all(blocks, everyone, split_axis=0, concat_axis=0, tiled=True)
        home = home.reshape(slab_count, cell_count, rows, own_regions, width)
        home = home.transpose(1, 3, 2, 0, 4).reshape(regions * rows, length)
        return home.astype(jnp.float32) * (1.0 / SEND_SCALE)

    home_x = back(along_x)
    home_y = back(along_y)
    sums = jnp.stack([excess_local, area_local, energy_local])
    sums, home_y = lax.optimization_barrier((sums, home_y))
    sums = jnp.broadcast_to(sums, (device_count, 3))
    sums = lax.all_to_all(sums, everyone, split_axis=0, concat_axis=0, tiled=True)
    field_x = matmul(home_x, sine, ((1,), (0,)))
    field_y = matmul(home_y, cosine, ((1,), (0,)))

    def pushed(field):
        sampled = lax.dot_general(
            x_intersect,
            field.astype(jnp.bfloat16),
            (((1,), (1,)), ((), ())),
            preferred_element_type=jnp.float32,
        )
        return jnp.sum(sampled * y_region.astype(jnp.float32), axis=1)

    partial = jnp.stack([pushed(field_x), pushed(field_y)])
    here, beneath = partial[:, : cells * cell_count], partial[:, cells * cell_count :]
    here = here + shifted(beneath, "slab", -1)
    here = here.reshape(2, cell_count, cells).transpose(1, 0, 2)
    cell_force = jnp.sum(lax.all_to_all(here, "cell", split_axis=0, concat_axis=0), axis=0)
    excess, area, energy = jnp.sum(sums, axis=0)
    shape = (regions, rows, length)
    return (field_x.reshape(shape), field_y.reshape(shape), cell_force, energy, excess / area)


INNER = 32
FINE = 48
LANES = 128
CODE_TOP = 32000.0


def trig(phase, length):
    angle = (phase % (4 * length)) * (math.pi / (2.0 * length))
    return np.cos(angle).astype(np.float32), np.sin(angle).astype(np.float32)


def small_tables(length):
    half = length // 2
    order = np.concatenate([2 * np.arange(half), 2 * np.arange(half) + 1])[None, :]
    coarse = np.arange(length // INNER)[:, None] * (2 * INNER)
    fine = 2 * np.arange(FINE)[:, None] + 1
    position = 2 * np.arange(half)[None, :] + 1
    freq_coarse = np.arange(half // INNER)[:, None] * (2 * INNER)
    freq_fine = (np.arange(2)[:, None, None] + 2 * np.arange(INNER)[None, :, None]) * position[None]
    return (
        trig(coarse * order, length)
        + trig(fine * order, length)
        + trig(freq_coarse * position, length)
        + trig(freq_fine, length)
    )


def split(value):
    high = value.astype(jnp.bfloat16)
    return high, (value - high.astype(jnp.float32)).astype(jnp.bfloat16)


def dot(left, right, contract=((1,), (0,))):
    return lax.dot_general(left, right, (contract, ((), ())), preferred_element_type=jnp.float32)


def overlap(steps, fraction, extent):
    high_edge = jnp.minimum(steps + 1.0, fraction + extent)
    return jnp.maximum(high_edge - jnp.maximum(steps, fraction), 0.0)


def row_iota(rows, columns):
    return lax.broadcasted_iota(jnp.int32, (rows, columns), 0).astype(jnp.float32)


def fold_rows(value):
    return jnp.sum(value.reshape(value.shape[0] // 8, 8, value.shape[1]), axis=0)


def fused_kernel(
    slab_count, length, cells, regions,
    cell_row, cell_col, cell_width, cell_height, cell_region, cell_offset,
    src_0, src_1, src_2, src_3, src_4, src_5, src_6, src_7,
    out_x, out_y, force, scalars,
    ccos, csin, fcos, fsin, gcos, gsin, hcos, hsin, table, field_x, field_y, cells_all, xch, xcl, ych, ycl, ysh, ysl, draw, foh, fol, hxh, hxl, hyh, hyl,
    send_buf, send_scale, recv_buf, recv_scale, rounded, xf, xg, carry, yown, ybelow,
    energy_acc, excess_acc, area_acc, scal_out, scal_in, part_own, part_below, part_sib, part_up,
    cell_send, cell_recv, data_send, data_recv, scale_send, scale_recv,
    scal_send, scal_recv, part_send, part_recv, out_sem, trig_sem,
):
    half = length // 2
    halves = slab_count // 2
    group = slab_count
    slab_rows = length // slab_count
    rows = slab_rows // 2
    both = 2 * cells
    device_count = 2 * slab_count
    slab = lax.axis_index("slab")
    core = lax.axis_index("cell")
    me = slab * 2 + core
    side = slab // halves
    spot = (slab % halves) * 2 + core
    f32, bf16 = jnp.float32, jnp.bfloat16

    def to(index):
        return (index // 2, index % 2)

    def neighbour(step):
        return ((slab + step // 2) % slab_count, (core + step) % 2)

    def cell_copy(step):
        return pltpu.make_async_remote_copy(
            src_ref=table, dst_ref=cells_all.at[me], send_sem=cell_send.at[step],
            recv_sem=cell_recv.at[me], device_id=neighbour(step),
            device_id_type=pl.DeviceIdType.MESH,
        )

    def cell_arrival(source):
        return pltpu.make_async_remote_copy(
            src_ref=table, dst_ref=cells_all.at[source], send_sem=cell_send.at[0],
            recv_sem=cell_recv.at[source], device_id=to((me + 1) % device_count),
            device_id_type=pl.DeviceIdType.MESH,
        )

    tables = [
        pltpu.make_async_copy(source, target, trig_sem.at[index])
        for index, (source, target) in enumerate(
            zip(
                (src_0, src_1, src_2, src_3, src_4, src_5, src_6, src_7),
                (ccos, csin, fcos, fsin, gcos, gsin, hcos, hsin),
            )
        )
    ]
    for copy in tables:
        copy.start()
    barrier = pltpu.get_barrier_semaphore()

    def greet(step, _):
        pl.semaphore_signal(
            barrier, inc=1, device_id=to((me + step) % device_count), device_id_type=pl.DeviceIdType.MESH
        )
        return 0

    lax.fori_loop(1, device_count, greet, 0)
    for index, ref in enumerate((cell_row, cell_col, cell_width, cell_height, cell_region)):
        table[pl.ds(index, 1), :] = ref[...].reshape(1, cells).astype(f32)
    table[5:7, :] = cell_offset[...]
    table[7:8, :] = jnp.zeros((1, cells), f32)
    pl.semaphore_wait(barrier, device_count - 1)

    def send_cells(step, _):
        cell_copy(step).start()
        return 0

    lax.fori_loop(1, device_count, send_cells, 0)
    cells_all[me] = table[...]
    for copy in tables:
        copy.wait()

    def rotate(cos_a, sin_a, cos_b, sin_b):
        return cos_a * cos_b - sin_a * sin_b, sin_a * cos_b + cos_a * sin_b

    def build_y(step, _):
        at = pl.ds(pl.multiple_of(step * INNER, INNER), INNER)
        row = pl.ds(side * (half // INNER) + step, 1)
        for parity in range(2):
            for part in range(half // 256):
                lanes = pl.ds(parity * half + part * 256, 256)
                out = pl.ds(part * 256, 256)
                cosine, sine = rotate(
                    ccos[row, lanes], csin[row, lanes], fcos[:INNER, lanes], fsin[:INNER, lanes]
                )
                ych[parity, at, out], ycl[parity, at, out] = split(cosine)
                ysh[parity, at, out], ysl[parity, at, out] = split(sine)
        return 0

    def build_x(step, high, low, pick):
        at = pl.ds(pl.multiple_of(step * INNER, INNER), INNER)
        row = pl.ds(step, 1)
        for parity in range(2):
            for part in range(half // 256):
                lanes = pl.ds(part * 256, 256)
                value = rotate(gcos[row, lanes], gsin[row, lanes], hcos[parity, :, lanes], hsin[parity, :, lanes])
                high[parity, at, lanes], low[parity, at, lanes] = split(value[pick])
        return 0

    lax.fori_loop(0, half // INNER, lambda s, c: build_x(s, xch, xcl, 0), 0)
    lax.fori_loop(0, half // INNER, build_y, 0)

    mine = pl.ds(pl.multiple_of(spot * LANES, LANES), LANES)
    coarse_rows = length // INNER
    for index, (fine_ref, coarse_ref) in enumerate(((fcos, ccos), (fsin, csin))):
        into = pl.ds(index * LANES, LANES)
        pad = jnp.zeros((LANES - FINE, LANES), f32)
        value = fine_ref[:, mine]
        high = value.astype(bf16).astype(f32)
        xf[into, :LANES] = jnp.concatenate([high, pad], 0).T.astype(bf16)
        xf[into, LANES:] = jnp.concatenate([value - high, pad], 0).T.astype(bf16)
        value = coarse_ref[:, mine]
        high = value.astype(bf16).astype(f32)
        xg[into, :] = jnp.concatenate([high, value - high], 0).T.astype(bf16)

    def slab_cells(index):
        block = jnp.concatenate([cells_all[2 * index], cells_all[2 * index + 1]], axis=1)
        return [block[i : i + 1, :] for i in range(7)]

    def spread(step, _):
        pair = [(slab + slab_count - 2 * step - back) % slab_count for back in range(2)]
        for index in pair:
            for part in range(2):

                @pl.when(2 * index + part != me)
                def _(source=2 * index + part):
                    cell_arrival(source).wait_recv()

        for index in pair:
            spread_slab(index)
        return 0

    def spread_slab(index):
        row, col, wide, high, region, off_x, off_y = slab_cells(index)
        upper = index // halves
        window = jnp.floor(col * (1.0 / INNER))
        local = col - window * INNER
        near = overlap(row_iota(FINE, both) - local, off_x, wide).astype(bf16)
        gap = jnp.zeros((LANES - FINE, both), bf16)
        hot = jnp.where(row_iota(coarse_rows, both) == window, 1.0, 0.0).astype(bf16)
        fine_part = dot(xf[...], jnp.concatenate([near, gap, near, gap], 0))
        coarse_part = dot(xg[...], jnp.concatenate([hot, hot], 0))
        along = fine_part[:LANES] * coarse_part[:LANES] - fine_part[LANES:] * coarse_part[LANES:]
        waves = jnp.concatenate(split(along), 0)
        start = (index * slab_rows).astype(f32)
        flip = upper.astype(f32)
        ladder = row_iota(slab_rows, both)
        place = start + ladder + flip * (slab_rows - 1.0 - 2.0 * ladder)
        tall = overlap(place - row, off_y, high).astype(bf16)
        flip_next = ((index + 1) // halves).astype(f32)
        steps = row_iota(8, both)
        place = start + slab_rows + steps + flip_next * (7.0 - 2.0 * steps)
        above = overlap(place - row, off_y, high)
        masks = [jnp.where(region == g, 1.0, 0.0) for g in range(regions)]
        above = jnp.concatenate([above * mask for mask in masks], 0).astype(bf16)
        stack = jnp.concatenate([tall * mask.astype(bf16) for mask in masks] + [above], 0)
        result = dot(stack, waves, ((1,), (1,)))
        result = result[:, :LANES] + result[:, LANES:]
        tile = index + upper * (2 * halves - 1 - 2 * index)
        base = pl.multiple_of(tile * slab_rows, slab_rows)
        for g in range(regions):
            lanes = pl.ds(g * LANES, LANES)
            draw[upper, pl.ds(base, slab_rows), lanes] = result[g * slab_rows : (g + 1) * slab_rows]
        carry[index] = result[regions * slab_rows :]

    lax.fori_loop(0, slab_count // 2, spread, 0)

    def hand_up(index, _):
        upper = index // halves
        tile = index + upper * (2 * halves - 1 - 2 * index)
        edge = pl.multiple_of(tile * slab_rows + upper * (slab_rows - 8), 8)
        for g in range(regions):
            lanes = pl.ds(g * LANES, LANES)
            draw[upper, pl.ds(edge, 8), lanes] += carry[index - 1, g * 8 : (g + 1) * 8, :]
        return 0

    lax.fori_loop(1, slab_count, hand_up, 0)

    def fold(step, _):
        at = pl.ds(pl.multiple_of(step * 64, 64), 64)
        lower, upper = draw[0, at, :], draw[1, at, :]
        foh[0, at, :], fol[0, at, :] = split(lower + upper)
        foh[1, at, :], fol[1, at, :] = split(lower - upper)
        return 0

    lax.fori_loop(0, half // 64, fold, 0)

    step_size = math.pi / length
    energy_acc[...] = jnp.zeros_like(energy_acc)
    chunk = 512
    kx = 2 * ((spot % halves) * LANES + lax.broadcasted_iota(jnp.int32, (chunk, LANES), 1)) + spot // halves
    kx = kx.astype(f32)

    def transform(step, _):
        parity = step // (half // chunk)
        first = (step % (half // chunk)) * chunk
        at = pl.ds(pl.multiple_of(first, chunk), chunk)
        high, low = xch[parity, at, :], xcl[parity, at, :]
        spectrum = dot(high, foh[parity]) + (dot(high, fol[parity]) + dot(low, foh[parity]))
        ky = (2 * (first + lax.broadcasted_iota(jnp.int32, (chunk, LANES), 0)) + parity).astype(f32)
        squared = kx * kx + ky * ky
        at_anchor = squared == 0.0
        scale = jnp.where(kx == 0.0, 1.0 / length, 2.0 / length) * jnp.where(ky == 0.0, 1.0 / length, 2.0 / length)
        weight = jnp.where(
            at_anchor, 0.0, scale / (step_size * step_size * jnp.where(at_anchor, 1.0, squared))
        )
        weight_x = weight * (step_size * kx)
        weight_y = weight * (step_size * ky)
        energy = energy_acc[...]
        for g in range(regions):
            lanes = pl.ds(g * LANES, LANES)
            part = spectrum[:, g * LANES : (g + 1) * LANES]
            hxh[parity, at, lanes], hxl[parity, at, lanes] = split(part * weight_x)
            hyh[parity, at, lanes], hyl[parity, at, lanes] = split(part * weight_y)
            energy += fold_rows(part * part * weight)
        energy_acc[...] = energy
        return 0

    lax.fori_loop(0, 2 * (half // chunk), transform, 0)

    def data_copy(index, target, source, place):
        return pltpu.make_async_remote_copy(
            src_ref=send_buf.at[index, target], dst_ref=recv_buf.at[index, source],
            send_sem=data_send.at[index, target], recv_sem=data_recv.at[index, source],
            device_id=to(side * group + place), device_id_type=pl.DeviceIdType.MESH,
        )

    def scale_copy(index, target, source, place):
        return pltpu.make_async_remote_copy(
            src_ref=send_scale.at[index, target], dst_ref=recv_scale.at[index, source],
            send_sem=scale_send.at[index, target], recv_sem=scale_recv.at[index, source],
            device_id=to(side * group + place), device_id_type=pl.DeviceIdType.MESH,
        )

    tiles = group // 4

    def inverse(step, _, index, th, tl, vh, vl):
        tile = (spot // 4 + step + 1) % tiles
        at = pl.ds(pl.multiple_of(tile * (4 * rows), 4 * rows), 4 * rows)
        value = None
        for parity in range(2):
            high, low = th[parity, at, :], tl[parity, at, :]
            term = dot(high, vh[parity]) + (dot(high, vl[parity]) + dot(low, vh[parity]))
            value = term if value is None else value + term
        for part in range(4):
            block = value[part * rows : (part + 1) * rows]
            top = jnp.maximum(jnp.max(jnp.abs(block), axis=0, keepdims=True), 1e-30)
            code = jnp.round(block * (CODE_TOP / top)).astype(jnp.int32).astype(jnp.int16)
            send_buf[index, tile * 4 + part] = code
            send_scale[index, tile * 4 + part] = jnp.broadcast_to(top * (1.0 / CODE_TOP), (2, regions * LANES))
        for part in range(4):
            target = tile * 4 + part

            @pl.when(target != spot)
            def _():
                data_copy(index, target, spot, target).start()
                scale_copy(index, target, spot, target).start()

            @pl.when(target == spot)
            def _():
                recv_buf[index, spot] = send_buf[index, spot]
                recv_scale[index, spot] = send_scale[index, spot]

        return 0

    for index, (th, tl, vh, vl) in enumerate(((ych, ycl, hxh, hxl), (ysh, ysl, hyh, hyl))):
        lax.fori_loop(
            0, tiles, functools.partial(inverse, index=index, th=th, tl=tl, vh=vh, vl=vl), 0
        )

    own = slab_cells(slab)
    under = slab_cells((slab + slab_count - 1) % slab_count)
    start = (slab * slab_rows + core * rows).astype(f32)
    for count, ref, (row, _, _, high, region, _, off_y) in ((rows, yown, own), (8, ybelow, under)):
        reach = overlap(start + row_iota(count, both) - row, off_y, high)
        for g in range(regions):
            ref[pl.ds(g * count, count), :] = jnp.where(region == g, reach, 0.0).astype(bf16)

    def columns(step, _):
        at = pl.ds(pl.multiple_of(step * 64, 64), 64)
        for part in range(2):
            spots = row_iota(64, both) + (step * 64 + part * half).astype(f32)
            for ref, (_, col, wide, _, _, off_x, _) in ((ych, own), (ycl, under)):
                ref[part, at, :] = overlap(spots - col, off_x, wide).astype(bf16)
        return 0

    lax.fori_loop(0, half // 64, columns, 0)
    excess_acc[...] = jnp.zeros_like(excess_acc)
    area_acc[...] = jnp.zeros_like(area_acc)

    def measure(step, _):
        part = step // (half // 256)
        at = pl.ds(pl.multiple_of((step % (half // 256)) * 256, 256), 256)
        density = dot(yown[...], ych[part, at, :], ((1,), (1,)))
        extra = dot(ybelow[...], ycl[part, at, :], ((1,), (1,)))
        excess, area = excess_acc[...], area_acc[...]
        for g in range(regions):
            block = density[g * rows : (g + 1) * rows]
            for piece in (block[:8] + extra[g * 8 : (g + 1) * 8], block[8:]):
                area += fold_rows(piece)
                excess += fold_rows(jnp.maximum(piece - 1.0, 0.0))
        excess_acc[...], area_acc[...] = excess, area
        return 0

    lax.fori_loop(0, length // 256, measure, 0)

    lane = lax.broadcasted_iota(jnp.int32, (8, LANES), 1)
    sums = jnp.where(lane == 0, jnp.sum(excess_acc[...]), 0.0)
    sums = jnp.where(lane == 1, jnp.sum(area_acc[...]), sums)
    sums = jnp.where(lane == 2, jnp.sum(energy_acc[...]) * (0.5 / (length * length)), sums)
    scal_out[...] = sums
    scal_in[me] = sums

    def scal_copy(step, source):
        return pltpu.make_async_remote_copy(
            src_ref=scal_out, dst_ref=scal_in.at[source], send_sem=scal_send.at[step],
            recv_sem=scal_recv.at[source], device_id=to((me + step) % device_count),
            device_id_type=pl.DeviceIdType.MESH,
        )

    def send_sums(step, _):
        scal_copy(step, me).start()
        return 0

    lax.fori_loop(1, device_count, send_sums, 0)
    lax.fori_loop(0, half // INNER, lambda s, c: build_x(s, ysh, ysl, 1), 0)

    def unpack(step, _, index):
        source = (spot + step) % group

        @pl.when(source != spot)
        def _():
            data_copy(index, source, source, source).wait_recv()
            scale_copy(index, source, source, source).wait_recv()

        across = source // 4
        lanes = pl.ds(pl.multiple_of((source % 4) * LANES, LANES), LANES)
        value = recv_buf[index, source].astype(jnp.int32).astype(f32) * recv_scale[index, source, :1, :]
        for g in range(regions):
            at = pl.ds(pl.multiple_of(across * (regions * rows) + g * rows, rows), rows)
            foh[index, at, lanes], fol[index, at, lanes] = split(value[:, g * LANES : (g + 1) * LANES])
        return 0

    high_rows = regions * rows
    mirror = LANES - 1 - lax.broadcasted_iota(jnp.int32, (high_rows, LANES), 1)
    wide = 256

    def finish(step, _, index, th, tl, out):
        at = pl.ds(pl.multiple_of(step * wide, wide), wide)
        sums = []
        for parity in range(2):
            total = None
            for block in range(2):
                pick = pl.ds((parity * 2 + block) * high_rows, high_rows)
                high, low = foh[index, pick, :], fol[index, pick, :]
                depth = pl.ds(block * 512, 512)
                left, right = th[parity, depth, at], tl[parity, depth, at]
                term = dot(high, left) + (dot(high, right) + dot(low, left))
                total = term if total is None else total + term
            sums.append(total)
        even, odd = sums
        straight = even + odd
        back = even - odd if index else odd - even
        rounded[:, at] = straight.astype(bf16)
        for g in range(regions):
            out[g, :, at] = straight[g * rows : (g + 1) * rows]
        for part in range(wide // LANES):
            tile = jnp.take_along_axis(
                back[:, part * LANES : (part + 1) * LANES], mirror, axis=1, mode="promise_in_bounds"
            )
            far = pl.ds(pl.multiple_of(length - (part + 1) * LANES - step * wide, LANES), LANES)
            rounded[:, far] = tile.astype(bf16)
            for g in range(regions):
                out[g, :, far] = tile[g * rows : (g + 1) * rows]
        return 0

    leaving = []
    for index, (th, tl, out, leave) in enumerate(((ysh, ysl, field_x, out_x), (xch, xcl, field_y, out_y))):
        lax.fori_loop(0, group, functools.partial(unpack, index=index), 0)
        lax.fori_loop(0, half // wide, functools.partial(finish, index=index, th=th, tl=tl, out=out), 0)
        leaving.append(pltpu.make_async_copy(out, leave, out_sem.at[index]))
        leaving[-1].start()
        low_rows = jnp.concatenate([out[g, :8, :] for g in range(regions)], 0).astype(bf16)
        total = dot(rounded[:, :half], ych[0]) + dot(rounded[:, half:], ych[1])
        extra = dot(low_rows[:, :half], ycl[0]) + dot(low_rows[:, half:], ycl[1])
        total = jnp.sum(total * yown[...].astype(f32), axis=0, keepdims=True)
        extra = jnp.sum(extra * ybelow[...].astype(f32), axis=0, keepdims=True)
        for part in range(2):
            part_own[part, pl.ds(index, 1), :] = total[:, part * cells : (part + 1) * cells]
            part_below[part, pl.ds(index, 1), :] = extra[:, part * cells : (part + 1) * cells]

    def sibling_copy():
        return pltpu.make_async_remote_copy(
            src_ref=part_own.at[1 - core], dst_ref=part_sib, send_sem=part_send.at[0],
            recv_sem=part_recv.at[0], device_id=(slab, 1 - core), device_id_type=pl.DeviceIdType.MESH,
        )

    def down_copy(part):
        return pltpu.make_async_remote_copy(
            src_ref=part_below.at[part], dst_ref=part_up, send_sem=part_send.at[1 + part],
            recv_sem=part_recv.at[1], device_id=(lax.max(slab - 1, 0), part),
            device_id_type=pl.DeviceIdType.MESH,
        )

    sibling_copy().start()

    @pl.when((core == 0) & (slab > 0))
    def _():
        down_copy(0).start()
        down_copy(1).start()

    def take_sums(step, _):
        scal_copy(step, (me + step) % device_count).wait_recv()
        return 0

    lax.fori_loop(1, device_count, take_sums, 0)
    total = scal_in[0]
    for source in range(1, device_count):
        total += scal_in[source]
    scalars[...] = jnp.where(lane == 3, total[:, :1] / total[:, 1:2], total)
    sibling_copy().wait_recv()
    force[...] = (part_own[core] + part_sib[...])[:2]

    @pl.when(slab < slab_count - 1)
    def _():
        down_copy(0).wait_recv()
        force[...] += part_up[:2, :]

    def drain(step, _):
        cell_copy(step).wait_send()
        scal_copy(step, me).wait_send()
        return 0

    lax.fori_loop(1, device_count, drain, 0)

    def drain_data(step, _):
        target = (spot + step) % group
        for index in range(2):
            data_copy(index, target, spot, target).wait_send()
            scale_copy(index, target, spot, target).wait_send()
        return 0

    lax.fori_loop(1, group, drain_data, 0)
    sibling_copy().wait_send()

    @pl.when((core == 0) & (slab > 0))
    def _():
        down_copy(0).wait_send()
        down_copy(1).wait_send()

    for copy in leaving:
        copy.wait()


def hand_out(in_x, in_y, in_force, in_scalars, out_x, out_y, force, energy, overflow, held, in_sem, out_sem):
    moves = []
    for index, (source, target) in enumerate(((in_x, out_x), (in_y, out_y))):
        for g in range(source.shape[0]):
            inward = pltpu.make_async_copy(source.at[g], held.at[index, g], in_sem.at[index, g])
            inward.start()
            moves.append((inward, pltpu.make_async_copy(held.at[index, g], target.at[g], out_sem.at[index, g])))
    for inward, outward in moves:
        inward.wait()
        outward.start()
    force[...] = in_force[...]
    energy[0, 0] = in_scalars[0, 2]
    overflow[0, 0] = in_scalars[0, 3]
    for _, outward in moves:
        outward.wait()


def fused_body(cell_row, cell_col, cell_width, cell_height, cell_region, cell_offset):
    slab_count = lax.axis_size("slab")
    length, regions = M, REGIONS
    cells = cell_row.shape[0]
    half, group = length // 2, slab_count
    device_count = 2 * slab_count
    rows = length // device_count
    f32, bf16 = jnp.float32, jnp.bfloat16
    consts = [jnp.asarray(t) for t in small_tables(length)]
    vmem = pltpu.VMEM
    basis = vmem((2, half, half), bf16)
    panel = vmem((2, half, regions * LANES), bf16)
    sems = pltpu.SemaphoreType.DMA
    scratch = (
        [vmem(t.shape, f32) for t in consts]
        + [vmem((8, cells), f32)]
        + [vmem((regions, rows, length), f32)] * 2
        + [vmem((device_count, 8, cells), f32)]
        + [basis] * 6
        + [vmem((2, half, regions * LANES), f32)]
        + [panel] * 6
        + [
            vmem((2, group, rows, regions * LANES), jnp.int16),
            vmem((2, group, 2, regions * LANES), f32),
            vmem((2, group, rows, regions * LANES), jnp.int16),
            vmem((2, group, 2, regions * LANES), f32),
            vmem((regions * rows, length), bf16),
            vmem((2 * LANES, 2 * LANES), bf16),
            vmem((2 * LANES, 2 * (length // INNER)), bf16),
            vmem((slab_count, 8 * regions, LANES), f32),
            vmem((regions * rows, 2 * cells), bf16),
            vmem((8 * regions, 2 * cells), bf16),
            vmem((8, LANES), f32),
            vmem((8, 256), f32),
            vmem((8, 256), f32),
            vmem((8, LANES), f32),
            vmem((device_count, 8, LANES), f32),
            vmem((2, 8, cells), f32),
            vmem((2, 8, cells), f32),
            vmem((8, cells), f32),
            vmem((8, cells), f32),
            sems((device_count,)),
            sems((device_count,)),
            sems((2, group)),
            sems((2, group)),
            sems((2, group)),
            sems((2, group)),
            sems((device_count,)),
            sems((device_count,)),
            sems((3,)),
            sems((2,)),
            sems((2,)),
            sems((len(consts),)),
        ]
    )
    whole = pl.BlockSpec(memory_space=vmem)
    anywhere = pl.BlockSpec(memory_space=pl.ANY)
    field = jax.ShapeDtypeStruct((regions, rows, length), f32)
    field_x, field_y, force, scalars = pl.pallas_call(
        functools.partial(fused_kernel, slab_count, length, cells, regions),
        out_shape=(
            field,
            field,
            jax.ShapeDtypeStruct((2, cells), f32),
            jax.ShapeDtypeStruct((8, LANES), f32),
        ),
        in_specs=[whole] * 6 + [anywhere] * len(consts),
        out_specs=(anywhere, anywhere, whole, whole),
        scratch_shapes=scratch,
        compiler_params=pltpu.CompilerParams(
            collective_id=0, has_side_effects=True, vmem_limit_bytes=67043328
        ),
    )(cell_row, cell_col, cell_width, cell_height, cell_region, cell_offset, *consts)
    number = pl.BlockSpec(memory_space=pltpu.SMEM)
    single = jax.ShapeDtypeStruct((1, 1), f32)
    field_x, field_y, force, energy, overflow = pl.pallas_call(
        hand_out,
        out_shape=(field, field, jax.ShapeDtypeStruct((2, cells), f32), single, single),
        in_specs=[anywhere, anywhere, whole, number],
        out_specs=(anywhere, anywhere, whole, number, number),
        scratch_shapes=[vmem((2, regions, rows, length), f32), sems((2, regions)), sems((2, regions))],
    )(field_x, field_y, force, scalars)
    return field_x, field_y, force, energy.reshape(()), overflow.reshape(())


def fits(mesh):
    slab_count = mesh.shape["slab"]
    return mesh.shape["cell"] == 2 and slab_count % 8 == 0 and M == slab_count * LANES


def solution(mesh):
    return jax.shard_map(
        fused_body if fits(mesh) else body,
        mesh=mesh,
        in_specs=(
            P(("slab", "cell")),
            P(("slab", "cell")),
            P(("slab", "cell")),
            P(("slab", "cell")),
            P(("slab", "cell")),
            P(None, ("slab", "cell")),
        ),
        out_specs=(
            P(None, ("slab", "cell"), None),
            P(None, ("slab", "cell"), None),
            P(None, ("slab", "cell")),
            P(),
            P(),
        ),
        check_vma=False,
    )
```

```python
import functools
import math

import jax
import jax.numpy as jnp
import numpy as np
from jax import lax
from jax.experimental import pallas as pl
from jax.experimental.pallas import tpu as pltpu
from jax.sharding import PartitionSpec as P

M = 2048
REGIONS = 4
SEND_SCALE = 0.125


def shifted(value, axis, steps):
    count = lax.axis_size(axis)
    first, last = (max(0, -steps), min(count, count - steps))
    return lax.ppermute(value, axis, [(source, source + steps) for source in range(first, last)])


def intersect(offset_bins, fraction, extent):
    high_edge = jnp.minimum(offset_bins + 1.0, fraction + extent)
    low_edge = jnp.maximum(offset_bins, fraction)
    return jnp.maximum(high_edge - low_edge, 0.0).astype(jnp.bfloat16)


def basis_tables(length):
    inner = 32
    outer = length // 2 // inner
    position = 2 * lax.iota(jnp.int32, length) + 1

    def small(freq):
        phase = freq[..., None] * position % (4 * length)
        angle = phase.astype(jnp.float32) * (math.pi / (2.0 * length))
        return jnp.cos(angle), jnp.sin(angle)

    coarse_cos, coarse_sin = small(2 * inner * lax.iota(jnp.int32, outer))
    parity = lax.iota(jnp.int32, 2)[:, None]
    fine_cos, fine_sin = small(2 * lax.iota(jnp.int32, inner)[None, :] + parity)
    coarse_cos, coarse_sin, fine_cos, fine_sin = lax.optimization_barrier(
        (coarse_cos, coarse_sin, fine_cos, fine_sin)
    )
    def build(left_a, right_a, left_b, right_b, sign):
        step_rows = min(4, outer) * inner

        def kernel(la, ra, lb, rb, out):
            step = pl.program_id(1)
            for part in range(step_rows // inner):
                at = pl.ds(step * (step_rows // inner) + part, 1)
                value = la[at, :] * ra[0] + sign * (lb[at, :] * rb[0])
                value = value * math.sqrt(2.0 / length)
                if part == 0:
                    first = (pl.program_id(0) == 0) & (step == 0)
                    here = lax.broadcasted_iota(jnp.int32, (inner, length), 0) == 0
                    value = jnp.where(first & here, value * math.sqrt(0.5), value)
                out[pl.ds(part * inner, inner), :] = value

        small_spec = pl.BlockSpec((outer, length), lambda p, i: (0, 0))
        fine_spec = pl.BlockSpec((1, inner, length), lambda p, i: (p, 0, 0))
        steps = outer * inner // step_rows
        return pl.pallas_call(
            kernel,
            out_shape=jax.ShapeDtypeStruct((length, length), jnp.float32),
            grid=(2, steps),
            in_specs=[small_spec, fine_spec, small_spec, fine_spec],
            out_specs=pl.BlockSpec((step_rows, length), lambda p, i: (p * steps + i, 0)),
            cost_estimate=pl.CostEstimate(
                flops=4 * length * length, bytes_accessed=4 * length * length, transcendentals=0
            ),
        )(left_a, right_a, left_b, right_b)

    cosine = build(coarse_cos, fine_cos, coarse_sin, fine_sin, -1.0)
    sine = build(coarse_sin, fine_cos, coarse_cos, fine_sin, 1.0)
    return cosine, sine


def frequency_order(index, length):
    half = length // 2
    return jnp.where(index < half, 2 * index, 2 * (index - half) + 1)


def matmul(left, right, contract):
    return lax.dot_general(
        left,
        right,
        (contract, ((), ())),
        precision=lax.Precision.HIGH,
        preferred_element_type=jnp.float32,
    )


def body(cell_row, cell_col, cell_width, cell_height, cell_region, cell_offset):
    slab_count = lax.axis_size("slab")
    cell_count = lax.axis_size("cell")
    slab_index = lax.axis_index("slab")
    cell_index = lax.axis_index("cell")
    device_count = slab_count * cell_count
    length = M
    regions = REGIONS
    own_regions = regions // cell_count
    rows = length // device_count
    width = length // slab_count
    cells = cell_row.shape[0]
    base_row = (slab_index * cell_count + cell_index) * rows
    everyone = ("slab", "cell")
    cosine, sine = basis_tables(length)

    table = jnp.concatenate(
        [jnp.stack([cell_row, cell_col, cell_width, cell_height, cell_region]).astype(jnp.float32), cell_offset]
    )
    slab_cells = lax.all_gather(table, "cell", axis=1, tiled=True)
    below = shifted(slab_cells, "slab", 1)
    seen = jnp.concatenate([slab_cells, below], axis=1)
    row, col, wide, high, region, off_x, off_y = [seen[i][:, None] for i in range(7)]
    natural = lax.iota(jnp.float32, length)[None, :]
    x_intersect = intersect(natural - col, off_x, wide)
    y_bins = base_row.astype(jnp.float32) + lax.iota(jnp.float32, rows)[None, :] - row
    y_intersect = intersect(y_bins, off_y, high)
    region_hot = region == lax.iota(jnp.float32, regions)[None, :]
    y_region = jnp.where(region_hot[:, :, None], y_intersect[:, None, :], jnp.bfloat16(0)).reshape(
        seen.shape[1], regions * rows
    )
    density = lax.dot_general(
        y_region, x_intersect, (((0,), (0,)), ((), ())), preferred_element_type=jnp.float32
    )
    excess_local = jnp.sum(jnp.maximum(density - 1.0, 0.0))
    area_local = jnp.sum(density)

    by_freq_x = matmul(density, cosine, ((1,), (1,)))
    outgoing = by_freq_x.reshape(cell_count, own_regions, rows, slab_count, width)
    outgoing = outgoing.astype(jnp.float16)
    outgoing = outgoing.transpose(3, 0, 2, 1, 4).reshape(device_count, rows, own_regions * width)
    crossed = lax.all_to_all(outgoing, everyone, split_axis=0, concat_axis=0, tiled=True)
    crossed, sine = lax.optimization_barrier((crossed, sine))
    crossed = crossed.reshape(length, own_regions * width).astype(jnp.float32)
    spectrum = matmul(crossed, cosine, ((0,), (1,)))

    ky_int = frequency_order(lax.iota(jnp.int32, length), length)[None, :]
    kx_int = frequency_order(slab_index * width + lax.iota(jnp.int32, width), length)
    kx_int = jnp.tile(kx_int, own_regions)[:, None]
    kx, ky = kx_int.astype(jnp.float32), ky_int.astype(jnp.float32)
    at_anchor = kx_int + ky_int == 0
    step_size = math.pi / length
    squared = kx * kx + ky * ky
    potential_hat = jnp.where(
        at_anchor, 0.0, spectrum / (step_size * step_size * jnp.where(at_anchor, 1.0, squared))
    )
    energy_local = jnp.sum(spectrum * potential_hat) / (length * length)
    along_x = matmul(potential_hat * (step_size * kx * SEND_SCALE), cosine, ((1,), (0,)))
    along_y = matmul(potential_hat * (step_size * ky * SEND_SCALE), sine, ((1,), (0,)))

    def back(along):
        blocks = along.astype(jnp.float16).T.reshape(device_count, rows, own_regions * width)
        home = lax.all_to_all(blocks, everyone, split_axis=0, concat_axis=0, tiled=True)
        home = home.reshape(slab_count, cell_count, rows, own_regions, width)
        home = home.transpose(1, 3, 2, 0, 4).reshape(regions * rows, length)
        return home.astype(jnp.float32) * (1.0 / SEND_SCALE)

    home_x = back(along_x)
    home_y = back(along_y)
    sums = jnp.stack([excess_local, area_local, energy_local])
    sums, home_y = lax.optimization_barrier((sums, home_y))
    sums = jnp.broadcast_to(sums, (device_count, 3))
    sums = lax.all_to_all(sums, everyone, split_axis=0, concat_axis=0, tiled=True)
    field_x = matmul(home_x, sine, ((1,), (0,)))
    field_y = matmul(home_y, cosine, ((1,), (0,)))

    def pushed(field):
        sampled = lax.dot_general(
            x_intersect,
            field.astype(jnp.bfloat16),
            (((1,), (1,)), ((), ())),
            preferred_element_type=jnp.float32,
        )
        return jnp.sum(sampled * y_region.astype(jnp.float32), axis=1)

    partial = jnp.stack([pushed(field_x), pushed(field_y)])
    here, beneath = partial[:, : cells * cell_count], partial[:, cells * cell_count :]
    here = here + shifted(beneath, "slab", -1)
    here = here.reshape(2, cell_count, cells).transpose(1, 0, 2)
    cell_force = jnp.sum(lax.all_to_all(here, "cell", split_axis=0, concat_axis=0), axis=0)
    excess, area, energy = jnp.sum(sums, axis=0)
    shape = (regions, rows, length)
    return (field_x.reshape(shape), field_y.reshape(shape), cell_force, energy, excess / area)


INNER = 32
FINE = 48
LANES = 128
CODE_TOP = 32000.0
NARROW = jnp.float8_e5m2
LIFT = 256.0
PANEL_SCALE = 64.0
HOME_SCALE = 16.0


def trig(phase, length):
    angle = (phase % (4 * length)) * (math.pi / (2.0 * length))
    return np.cos(angle).astype(np.float32), np.sin(angle).astype(np.float32)


def small_tables(length):
    half = length // 2
    order = np.concatenate([2 * np.arange(half), 2 * np.arange(half) + 1])[None, :]
    coarse = np.arange(length // INNER)[:, None] * (2 * INNER)
    fine = 2 * np.arange(FINE)[:, None] + 1
    position = 2 * np.arange(half)[None, :] + 1
    freq_coarse = np.arange(half // INNER)[:, None] * (2 * INNER)
    freq_fine = (np.arange(2)[:, None, None] + 2 * np.arange(INNER)[None, :, None]) * position[None]
    return (
        trig(coarse * order, length)
        + trig(fine * order, length)
        + trig(freq_coarse * position, length)
        + trig(freq_fine, length)
    )


def split(value):
    high = value.astype(jnp.bfloat16)
    return high, (value - high.astype(jnp.float32)).astype(jnp.bfloat16)


def put(high, narrow, at, value, scale=1.0):
    head = value.astype(jnp.bfloat16)
    high[at] = head
    rest = value - head.astype(jnp.float32)
    narrow[(0,) + at] = (value * scale if scale != 1.0 else value).astype(NARROW)
    narrow[(1,) + at] = (rest * (LIFT * scale)).astype(NARROW)


def dot(left, right, contract=((1,), (0,))):
    return lax.dot_general(left, right, (contract, ((), ())), preferred_element_type=jnp.float32)


def overlap(steps, fraction, extent):
    high_edge = jnp.minimum(steps + 1.0, fraction + extent)
    return jnp.maximum(high_edge - jnp.maximum(steps, fraction), 0.0)


def row_iota(rows, columns):
    return lax.broadcasted_iota(jnp.int32, (rows, columns), 0).astype(jnp.float32)


def fold_rows(value):
    return jnp.sum(value.reshape(value.shape[0] // 8, 8, value.shape[1]), axis=0)


def fused_kernel(
    slab_count, length, cells, regions,
    cell_row, cell_col, cell_width, cell_height, cell_region, cell_offset,
    src_0, src_1, src_2, src_3, src_4, src_5, src_6, src_7,
    out_x, out_y, force, scalars,
    ccos, csin, fcos, fsin, gcos, gsin, hcos, hsin, table, field_x, field_y, cells_all, xch, xcl, ych, ycl, ysh, ysl, draw, foh, fol, hxh, hxl, hyh, hyl,
    send_buf, send_scale, recv_buf, recv_scale, rounded, xf, xg, carry, yown, ybelow,
    low_columns, energy_acc, excess_acc, area_acc, scal_out, scal_in, part_own, part_below, part_sib, part_up,
    cell_send, cell_recv, data_send, data_recv, scale_send, scale_recv,
    scal_send, scal_recv, part_send, part_recv, out_sem, trig_sem,
):
    half = length // 2
    halves = slab_count // 2
    group = slab_count
    slab_rows = length // slab_count
    rows = slab_rows // 2
    both = 2 * cells
    device_count = 2 * slab_count
    slab = lax.axis_index("slab")
    core = lax.axis_index("cell")
    me = slab * 2 + core
    side = slab // halves
    spot = (slab % halves) * 2 + core
    f32, bf16 = jnp.float32, jnp.bfloat16

    def to(index):
        return (index // 2, index % 2)

    def neighbour(step):
        return ((slab + step // 2) % slab_count, (core + step) % 2)

    def cell_copy(step):
        return pltpu.make_async_remote_copy(
            src_ref=table, dst_ref=cells_all.at[me], send_sem=cell_send.at[step],
            recv_sem=cell_recv.at[me], device_id=neighbour(step),
            device_id_type=pl.DeviceIdType.MESH,
        )

    def cell_arrival(source):
        return pltpu.make_async_remote_copy(
            src_ref=table, dst_ref=cells_all.at[source], send_sem=cell_send.at[0],
            recv_sem=cell_recv.at[source], device_id=to((me + 1) % device_count),
            device_id_type=pl.DeviceIdType.MESH,
        )

    tables = [
        pltpu.make_async_copy(source, target, trig_sem.at[index])
        for index, (source, target) in enumerate(
            zip(
                (src_0, src_1, src_2, src_3, src_4, src_5, src_6, src_7),
                (ccos, csin, fcos, fsin, gcos, gsin, hcos, hsin),
            )
        )
    ]
    for copy in tables:
        copy.start()
    barrier = pltpu.get_barrier_semaphore()

    def greet(step, _):
        pl.semaphore_signal(
            barrier, inc=1, device_id=to((me + step) % device_count), device_id_type=pl.DeviceIdType.MESH
        )
        return 0

    lax.fori_loop(1, device_count, greet, 0)
    for index, ref in enumerate((cell_row, cell_col, cell_width, cell_height, cell_region)):
        table[pl.ds(index, 1), :] = ref[...].reshape(1, cells).astype(f32)
    table[5:7, :] = cell_offset[...]
    table[7:8, :] = jnp.zeros((1, cells), f32)
    pl.semaphore_wait(barrier, device_count - 1)

    def send_cells(step, _):
        cell_copy(step).start()
        return 0

    lax.fori_loop(1, device_count, send_cells, 0)
    cells_all[me] = table[...]
    for copy in tables:
        copy.wait()

    def rotate(cos_a, sin_a, cos_b, sin_b):
        return cos_a * cos_b - sin_a * sin_b, sin_a * cos_b + cos_a * sin_b

    def build_y(step, _):
        at = pl.ds(pl.multiple_of(step * INNER, INNER), INNER)
        row = pl.ds(side * (half // INNER) + step, 1)
        for parity in range(2):
            for part in range(half // 256):
                lanes = pl.ds(parity * half + part * 256, 256)
                out = pl.ds(part * 256, 256)
                cosine, sine = rotate(
                    ccos[row, lanes], csin[row, lanes], fcos[:INNER, lanes], fsin[:INNER, lanes]
                )
                put(ych, ycl, (parity, at, out), cosine)
                put(ysh, ysl, (parity, at, out), sine)
        return 0

    def build_x(step, high, low, pick):
        at = pl.ds(pl.multiple_of(step * INNER, INNER), INNER)
        row = pl.ds(step, 1)
        for parity in range(2):
            for part in range(half // 256):
                lanes = pl.ds(part * 256, 256)
                value = rotate(gcos[row, lanes], gsin[row, lanes], hcos[parity, :, lanes], hsin[parity, :, lanes])
                put(high, low, (parity, at, lanes), value[pick])
        return 0

    lax.fori_loop(0, half // INNER, lambda s, c: build_x(s, xch, xcl, 0), 0)
    lax.fori_loop(0, half // INNER, build_y, 0)

    mine = pl.ds(pl.multiple_of(spot * LANES, LANES), LANES)
    coarse_rows = length // INNER
    for index, (fine_ref, coarse_ref) in enumerate(((fcos, ccos), (fsin, csin))):
        into = pl.ds(index * LANES, LANES)
        pad = jnp.zeros((LANES - FINE, LANES), f32)
        value = fine_ref[:, mine]
        high = value.astype(bf16).astype(f32)
        xf[into, :LANES] = jnp.concatenate([high, pad], 0).T.astype(bf16)
        xf[into, LANES:] = jnp.concatenate([value - high, pad], 0).T.astype(bf16)
        value = coarse_ref[:, mine]
        high = value.astype(bf16).astype(f32)
        xg[into, :] = jnp.concatenate([high, value - high], 0).T.astype(bf16)

    def slab_cells(index):
        block = jnp.concatenate([cells_all[2 * index], cells_all[2 * index + 1]], axis=1)
        return [block[i : i + 1, :] for i in range(7)]

    def spread(step, _):
        pair = [(slab + slab_count - 2 * step - back) % slab_count for back in range(2)]
        for index in pair:
            for part in range(2):

                @pl.when(2 * index + part != me)
                def _(source=2 * index + part):
                    cell_arrival(source).wait_recv()

        for index in pair:
            spread_slab(index)
        return 0

    def spread_slab(index):
        row, col, wide, high, region, off_x, off_y = slab_cells(index)
        upper = index // halves
        window = jnp.floor(col * (1.0 / INNER))
        local = col - window * INNER
        near = overlap(row_iota(FINE, both) - local, off_x, wide).astype(bf16)
        gap = jnp.zeros((LANES - FINE, both), bf16)
        hot = jnp.where(row_iota(coarse_rows, both) == window, 1.0, 0.0).astype(bf16)
        fine_part = dot(xf[...], jnp.concatenate([near, gap, near, gap], 0))
        coarse_part = dot(xg[...], jnp.concatenate([hot, hot], 0))
        along = fine_part[:LANES] * coarse_part[:LANES] - fine_part[LANES:] * coarse_part[LANES:]
        waves = jnp.concatenate(split(along), 0)
        start = (index * slab_rows).astype(f32)
        flip = upper.astype(f32)
        ladder = row_iota(slab_rows, both)
        place = start + ladder + flip * (slab_rows - 1.0 - 2.0 * ladder)
        tall = overlap(place - row, off_y, high).astype(bf16)
        flip_next = ((index + 1) // halves).astype(f32)
        steps = row_iota(8, both)
        place = start + slab_rows + steps + flip_next * (7.0 - 2.0 * steps)
        above = overlap(place - row, off_y, high)
        masks = [jnp.where(region == g, 1.0, 0.0) for g in range(regions)]
        above = jnp.concatenate([above * mask for mask in masks], 0).astype(bf16)
        stack = jnp.concatenate([tall * mask.astype(bf16) for mask in masks] + [above], 0)
        result = dot(stack, waves, ((1,), (1,)))
        result = result[:, :LANES] + result[:, LANES:]
        tile = index + upper * (2 * halves - 1 - 2 * index)
        base = pl.multiple_of(tile * slab_rows, slab_rows)
        for g in range(regions):
            lanes = pl.ds(g * LANES, LANES)
            draw[upper, pl.ds(base, slab_rows), lanes] = result[g * slab_rows : (g + 1) * slab_rows]
        carry[index] = result[regions * slab_rows :]

    lax.fori_loop(0, slab_count // 2, spread, 0)

    def hand_up(index, _):
        upper = index // halves
        tile = index + upper * (2 * halves - 1 - 2 * index)
        edge = pl.multiple_of(tile * slab_rows + upper * (slab_rows - 8), 8)
        for g in range(regions):
            lanes = pl.ds(g * LANES, LANES)
            draw[upper, pl.ds(edge, 8), lanes] += carry[index - 1, g * 8 : (g + 1) * 8, :]
        return 0

    lax.fori_loop(1, slab_count, hand_up, 0)

    def fold(step, _):
        at = pl.ds(pl.multiple_of(step * 64, 64), 64)
        lower, upper = draw[0, at, :], draw[1, at, :]
        every = slice(None)
        put(foh, fol, (0, at, every), lower + upper)
        put(foh, fol, (1, at, every), lower - upper)
        return 0

    lax.fori_loop(0, half // 64, fold, 0)

    step_size = math.pi / length
    energy_acc[...] = jnp.zeros_like(energy_acc)
    chunk = 512
    kx = 2 * ((spot % halves) * LANES + lax.broadcasted_iota(jnp.int32, (chunk, LANES), 1)) + spot // halves
    kx = kx.astype(f32)

    def transform(step, _):
        parity = step // (half // chunk)
        first = (step % (half // chunk)) * chunk
        at = pl.ds(pl.multiple_of(first, chunk), chunk)
        cross = dot(xcl[0, parity, at, :], fol[1, parity]) + dot(xcl[1, parity, at, :], fol[0, parity])
        spectrum = dot(xch[parity, at, :], foh[parity]) + cross * (1.0 / LIFT)
        ky = (2 * (first + lax.broadcasted_iota(jnp.int32, (chunk, LANES), 0)) + parity).astype(f32)
        squared = kx * kx + ky * ky
        at_anchor = squared == 0.0
        scale = jnp.where(kx == 0.0, 1.0 / length, 2.0 / length) * jnp.where(ky == 0.0, 1.0 / length, 2.0 / length)
        weight = jnp.where(
            at_anchor, 0.0, scale / (step_size * step_size * jnp.where(at_anchor, 1.0, squared))
        )
        weight_x = weight * (step_size * kx)
        weight_y = weight * (step_size * ky)
        energy = energy_acc[...]
        for g in range(regions):
            lanes = pl.ds(g * LANES, LANES)
            part = spectrum[:, g * LANES : (g + 1) * LANES]
            put(hxh, hxl, (parity, at, lanes), part * weight_x, PANEL_SCALE)
            put(hyh, hyl, (parity, at, lanes), part * weight_y, PANEL_SCALE)
            energy += fold_rows(part * part * weight)
        energy_acc[...] = energy
        return 0

    lax.fori_loop(0, 2 * (half // chunk), transform, 0)

    def data_copy(index, target, source, place):
        return pltpu.make_async_remote_copy(
            src_ref=send_buf.at[index, target], dst_ref=recv_buf.at[index, source],
            send_sem=data_send.at[index, target], recv_sem=data_recv.at[index, source],
            device_id=to(side * group + place), device_id_type=pl.DeviceIdType.MESH,
        )

    def scale_copy(index, target, source, place):
        return pltpu.make_async_remote_copy(
            src_ref=send_scale.at[index, target], dst_ref=recv_scale.at[index, source],
            send_sem=scale_send.at[index, target], recv_sem=scale_recv.at[index, source],
            device_id=to(side * group + place), device_id_type=pl.DeviceIdType.MESH,
        )

    tiles = group // 4

    def inverse(step, _, index, th, tl, vh, vl):
        tile = (spot // 4 + step + 1) % tiles
        at = pl.ds(pl.multiple_of(tile * (4 * rows), 4 * rows), 4 * rows)
        value = cross = None
        for parity in range(2):
            term = dot(th[parity, at, :], vh[parity])
            more = dot(tl[0, parity, at, :], vl[1, parity]) + dot(tl[1, parity, at, :], vl[0, parity])
            value = term if value is None else value + term
            cross = more if cross is None else cross + more
        value = value + cross * (1.0 / (LIFT * PANEL_SCALE))
        for part in range(4):
            block = value[part * rows : (part + 1) * rows]
            top = jnp.maximum(jnp.max(jnp.abs(block), axis=0, keepdims=True), 1e-30)
            code = jnp.round(block * (CODE_TOP / top)).astype(jnp.int32).astype(jnp.int16)
            send_buf[index, tile * 4 + part] = code
            send_scale[index, tile * 4 + part] = jnp.broadcast_to(top * (1.0 / CODE_TOP), (2, regions * LANES))
        for part in range(4):
            target = tile * 4 + part

            @pl.when(target != spot)
            def _():
                data_copy(index, target, spot, target).start()
                scale_copy(index, target, spot, target).start()

            @pl.when(target == spot)
            def _():
                recv_buf[index, spot] = send_buf[index, spot]
                recv_scale[index, spot] = send_scale[index, spot]

        return 0

    for index, (th, tl, vh, vl) in enumerate(((ych, ycl, hxh, hxl), (ysh, ysl, hyh, hyl))):
        lax.fori_loop(
            0, tiles, functools.partial(inverse, index=index, th=th, tl=tl, vh=vh, vl=vl), 0
        )

    own = slab_cells(slab)
    under = slab_cells((slab + slab_count - 1) % slab_count)
    start = (slab * slab_rows + core * rows).astype(f32)
    for count, ref, (row, _, _, high, region, _, off_y) in ((rows, yown, own), (8, ybelow, under)):
        reach = overlap(start + row_iota(count, both) - row, off_y, high)
        for g in range(regions):
            ref[pl.ds(g * count, count), :] = jnp.where(region == g, reach, 0.0).astype(bf16)

    def columns(step, _):
        at = pl.ds(pl.multiple_of(step * 64, 64), 64)
        for part in range(2):
            spots = row_iota(64, both) + (step * 64 + part * half).astype(f32)
            for ref, (_, col, wide, _, _, off_x, _) in ((ych, own), (low_columns, under)):
                ref[part, at, :] = overlap(spots - col, off_x, wide).astype(bf16)
        return 0

    lax.fori_loop(0, half // 64, columns, 0)
    excess_acc[...] = jnp.zeros_like(excess_acc)
    area_acc[...] = jnp.zeros_like(area_acc)

    def measure(step, _):
        part = step // (half // 256)
        at = pl.ds(pl.multiple_of((step % (half // 256)) * 256, 256), 256)
        density = dot(yown[...], ych[part, at, :], ((1,), (1,)))
        extra = dot(ybelow[...], low_columns[part, at, :], ((1,), (1,)))
        excess, area = excess_acc[...], area_acc[...]
        for g in range(regions):
            block = density[g * rows : (g + 1) * rows]
            for piece in (block[:8] + extra[g * 8 : (g + 1) * 8], block[8:]):
                area += fold_rows(piece)
                excess += fold_rows(jnp.maximum(piece - 1.0, 0.0))
        excess_acc[...], area_acc[...] = excess, area
        return 0

    lax.fori_loop(0, length // 256, measure, 0)

    lane = lax.broadcasted_iota(jnp.int32, (8, LANES), 1)
    sums = jnp.where(lane == 0, jnp.sum(excess_acc[...]), 0.0)
    sums = jnp.where(lane == 1, jnp.sum(area_acc[...]), sums)
    sums = jnp.where(lane == 2, jnp.sum(energy_acc[...]) * (0.5 / (length * length)), sums)
    scal_out[...] = sums
    scal_in[me] = sums

    def scal_copy(step, source):
        return pltpu.make_async_remote_copy(
            src_ref=scal_out, dst_ref=scal_in.at[source], send_sem=scal_send.at[step],
            recv_sem=scal_recv.at[source], device_id=to((me + step) % device_count),
            device_id_type=pl.DeviceIdType.MESH,
        )

    def send_sums(step, _):
        scal_copy(step, me).start()
        return 0

    lax.fori_loop(1, device_count, send_sums, 0)
    lax.fori_loop(0, half // INNER, lambda s, c: build_x(s, ysh, ysl, 1), 0)

    def unpack(step, _, index):
        source = (spot + step) % group

        @pl.when(source != spot)
        def _():
            data_copy(index, source, source, source).wait_recv()
            scale_copy(index, source, source, source).wait_recv()

        across = source // 4
        lanes = pl.ds(pl.multiple_of((source % 4) * LANES, LANES), LANES)
        value = recv_buf[index, source].astype(jnp.int32).astype(f32) * recv_scale[index, source, :1, :]
        for g in range(regions):
            at = pl.ds(pl.multiple_of(across * (regions * rows) + g * rows, rows), rows)
            put(foh, fol, (index, at, lanes), value[:, g * LANES : (g + 1) * LANES], HOME_SCALE)
        return 0

    high_rows = regions * rows
    mirror = LANES - 1 - lax.broadcasted_iota(jnp.int32, (high_rows, LANES), 1)
    wide = 256

    def finish(step, _, index, th, tl, out):
        at = pl.ds(pl.multiple_of(step * wide, wide), wide)
        sums = []
        for parity in range(2):
            total = cross = None
            for block in range(2):
                pick = pl.ds((parity * 2 + block) * high_rows, high_rows)
                depth = pl.ds(block * 512, 512)
                term = dot(foh[index, pick, :], th[parity, depth, at])
                more = dot(fol[0, index, pick, :], tl[1, parity, depth, at])
                more += dot(fol[1, index, pick, :], tl[0, parity, depth, at])
                total = term if total is None else total + term
                cross = more if cross is None else cross + more
            sums.append(total + cross * (1.0 / (LIFT * HOME_SCALE)))
        even, odd = sums
        straight = even + odd
        back = even - odd if index else odd - even
        rounded[:, at] = straight.astype(bf16)
        for g in range(regions):
            out[g, :, at] = straight[g * rows : (g + 1) * rows]
        for part in range(wide // LANES):
            tile = jnp.take_along_axis(
                back[:, part * LANES : (part + 1) * LANES], mirror, axis=1, mode="promise_in_bounds"
            )
            far = pl.ds(pl.multiple_of(length - (part + 1) * LANES - step * wide, LANES), LANES)
            rounded[:, far] = tile.astype(bf16)
            for g in range(regions):
                out[g, :, far] = tile[g * rows : (g + 1) * rows]
        return 0

    leaving = []
    for index, (th, tl, out, leave) in enumerate(((ysh, ysl, field_x, out_x), (xch, xcl, field_y, out_y))):
        lax.fori_loop(0, group, functools.partial(unpack, index=index), 0)
        lax.fori_loop(0, half // wide, functools.partial(finish, index=index, th=th, tl=tl, out=out), 0)
        leaving.append(pltpu.make_async_copy(out, leave, out_sem.at[index]))
        leaving[-1].start()
        low_rows = jnp.concatenate([out[g, :8, :] for g in range(regions)], 0).astype(bf16)
        total = dot(rounded[:, :half], ych[0]) + dot(rounded[:, half:], ych[1])
        extra = dot(low_rows[:, :half], low_columns[0]) + dot(low_rows[:, half:], low_columns[1])
        total = jnp.sum(total * yown[...].astype(f32), axis=0, keepdims=True)
        extra = jnp.sum(extra * ybelow[...].astype(f32), axis=0, keepdims=True)
        for part in range(2):
            part_own[part, pl.ds(index, 1), :] = total[:, part * cells : (part + 1) * cells]
            part_below[part, pl.ds(index, 1), :] = extra[:, part * cells : (part + 1) * cells]

    def sibling_copy():
        return pltpu.make_async_remote_copy(
            src_ref=part_own.at[1 - core], dst_ref=part_sib, send_sem=part_send.at[0],
            recv_sem=part_recv.at[0], device_id=(slab, 1 - core), device_id_type=pl.DeviceIdType.MESH,
        )

    def down_copy(part):
        return pltpu.make_async_remote_copy(
            src_ref=part_below.at[part], dst_ref=part_up, send_sem=part_send.at[1 + part],
            recv_sem=part_recv.at[1], device_id=(lax.max(slab - 1, 0), part),
            device_id_type=pl.DeviceIdType.MESH,
        )

    sibling_copy().start()

    @pl.when((core == 0) & (slab > 0))
    def _():
        down_copy(0).start()
        down_copy(1).start()

    def take_sums(step, _):
        scal_copy(step, (me + step) % device_count).wait_recv()
        return 0

    lax.fori_loop(1, device_count, take_sums, 0)
    total = scal_in[0]
    for source in range(1, device_count):
        total += scal_in[source]
    scalars[...] = jnp.where(lane == 3, total[:, :1] / total[:, 1:2], total)
    sibling_copy().wait_recv()
    force[...] = (part_own[core] + part_sib[...])[:2]

    @pl.when(slab < slab_count - 1)
    def _():
        down_copy(0).wait_recv()
        force[...] += part_up[:2, :]

    def drain(step, _):
        cell_copy(step).wait_send()
        scal_copy(step, me).wait_send()
        return 0

    lax.fori_loop(1, device_count, drain, 0)

    def drain_data(step, _):
        target = (spot + step) % group
        for index in range(2):
            data_copy(index, target, spot, target).wait_send()
            scale_copy(index, target, spot, target).wait_send()
        return 0

    lax.fori_loop(1, group, drain_data, 0)
    sibling_copy().wait_send()

    @pl.when((core == 0) & (slab > 0))
    def _():
        down_copy(0).wait_send()
        down_copy(1).wait_send()

    for copy in leaving:
        copy.wait()


def hand_out(in_x, in_y, in_force, in_scalars, out_x, out_y, force, energy, overflow, held, in_sem, out_sem):
    moves = []
    for index, (source, target) in enumerate(((in_x, out_x), (in_y, out_y))):
        for g in range(source.shape[0]):
            inward = pltpu.make_async_copy(source.at[g], held.at[index, g], in_sem.at[index, g])
            inward.start()
            moves.append((inward, pltpu.make_async_copy(held.at[index, g], target.at[g], out_sem.at[index, g])))
    for inward, outward in moves:
        inward.wait()
        outward.start()
    force[...] = in_force[...]
    energy[0, 0] = in_scalars[0, 2]
    overflow[0, 0] = in_scalars[0, 3]
    for _, outward in moves:
        outward.wait()


def fused_body(cell_row, cell_col, cell_width, cell_height, cell_region, cell_offset):
    slab_count = lax.axis_size("slab")
    length, regions = M, REGIONS
    cells = cell_row.shape[0]
    half, group = length // 2, slab_count
    device_count = 2 * slab_count
    rows = length // device_count
    f32, bf16 = jnp.float32, jnp.bfloat16
    consts = [jnp.asarray(t) for t in small_tables(length)]
    vmem = pltpu.VMEM
    basis = vmem((2, half, half), bf16)
    panel = vmem((2, half, regions * LANES), bf16)
    basis_cross = vmem((2, 2, half, half), NARROW)
    panel_cross = vmem((2, 2, half, regions * LANES), NARROW)
    sems = pltpu.SemaphoreType.DMA
    scratch = (
        [vmem(t.shape, f32) for t in consts]
        + [vmem((8, cells), f32)]
        + [vmem((regions, rows, length), f32)] * 2
        + [vmem((device_count, 8, cells), f32)]
        + [basis, basis_cross] * 3
        + [vmem((2, half, regions * LANES), f32)]
        + [panel, panel_cross] * 3
        + [
            vmem((2, group, rows, regions * LANES), jnp.int16),
            vmem((2, group, 2, regions * LANES), f32),
            vmem((2, group, rows, regions * LANES), jnp.int16),
            vmem((2, group, 2, regions * LANES), f32),
            vmem((regions * rows, length), bf16),
            vmem((2 * LANES, 2 * LANES), bf16),
            vmem((2 * LANES, 2 * (length // INNER)), bf16),
            vmem((slab_count, 8 * regions, LANES), f32),
            vmem((regions * rows, 2 * cells), bf16),
            vmem((8 * regions, 2 * cells), bf16),
            basis,
            vmem((8, LANES), f32),
            vmem((8, 256), f32),
            vmem((8, 256), f32),
            vmem((8, LANES), f32),
            vmem((device_count, 8, LANES), f32),
            vmem((2, 8, cells), f32),
            vmem((2, 8, cells), f32),
            vmem((8, cells), f32),
            vmem((8, cells), f32),
            sems((device_count,)),
            sems((device_count,)),
            sems((2, group)),
            sems((2, group)),
            sems((2, group)),
            sems((2, group)),
            sems((device_count,)),
            sems((device_count,)),
            sems((3,)),
            sems((2,)),
            sems((2,)),
            sems((len(consts),)),
        ]
    )
    whole = pl.BlockSpec(memory_space=vmem)
    anywhere = pl.BlockSpec(memory_space=pl.ANY)
    field = jax.ShapeDtypeStruct((regions, rows, length), f32)
    field_x, field_y, force, scalars = pl.pallas_call(
        functools.partial(fused_kernel, slab_count, length, cells, regions),
        out_shape=(
            field,
            field,
            jax.ShapeDtypeStruct((2, cells), f32),
            jax.ShapeDtypeStruct((8, LANES), f32),
        ),
        in_specs=[whole] * 6 + [anywhere] * len(consts),
        out_specs=(anywhere, anywhere, whole, whole),
        scratch_shapes=scratch,
        compiler_params=pltpu.CompilerParams(
            collective_id=0, has_side_effects=True, vmem_limit_bytes=67043328
        ),
    )(cell_row, cell_col, cell_width, cell_height, cell_region, cell_offset, *consts)
    number = pl.BlockSpec(memory_space=pltpu.SMEM)
    single = jax.ShapeDtypeStruct((1, 1), f32)
    field_x, field_y, force, energy, overflow = pl.pallas_call(
        hand_out,
        out_shape=(field, field, jax.ShapeDtypeStruct((2, cells), f32), single, single),
        in_specs=[anywhere, anywhere, whole, number],
        out_specs=(anywhere, anywhere, whole, number, number),
        scratch_shapes=[vmem((2, regions, rows, length), f32), sems((2, regions)), sems((2, regions))],
    )(field_x, field_y, force, scalars)
    return field_x, field_y, force, energy.reshape(()), overflow.reshape(())


def fits(mesh):
    slab_count = mesh.shape["slab"]
    return mesh.shape["cell"] == 2 and slab_count % 8 == 0 and M == slab_count * LANES


def solution(mesh):
    return jax.shard_map(
        fused_body if fits(mesh) else body,
        mesh=mesh,
        in_specs=(
            P(("slab", "cell")),
            P(("slab", "cell")),
            P(("slab", "cell")),
            P(("slab", "cell")),
            P(("slab", "cell")),
            P(None, ("slab", "cell")),
        ),
        out_specs=(
            P(None, ("slab", "cell"), None),
            P(None, ("slab", "cell"), None),
            P(None, ("slab", "cell")),
            P(),
            P(),
        ),
        check_vma=False,
    )
```
